32 devices in a mesh: rep: 2 (over y), gx: 16 (over z, x, core).
Axes of the slice: x: 2, y: 2, z: 4, core: 2. Of those that a mesh axis runs over, the one named last changes fastest.
Arguments:
- positions: float32 [3, 49152], P(None, ('rep', 'gx')), parts along dimension 1, may hold values from 0 to 96
- velocities: float32 [3, 49152], P(None, ('rep', 'gx')), parts along dimension 1, may hold values from -9 to 9
- atom_params: float32 [4, 49152], P(None, ('rep', 'gx')), parts along dimension 1, may hold values from -1 to 2, as said below
- pair_list: int32 [3, 540672], P(None, ('rep', 'gx')), parts along dimension 1, may hold values from 0 to 479, as said below
- pair_count: int32 [32], P(('rep', 'gx')), parts along dimension 0, may hold values from 2112 to 16896, as said below
- exclusion: int32 [4, 540672], P(None, ('rep', 'gx')), parts along dimension 1, may hold values from 0 to 65535, as said below
- halo_far: int32 [3072], P(('rep', 'gx')), parts along dimension 0, may hold values from 0 to 191, as said below
- box_lengths: float32 [6], P('rep'), parts along dimension 0, may hold values from 12 to 96
- extended_variables: float32 [8], P('rep'), parts along dimension 0, may hold values from -0.3 to 0.3
Outputs:
- forces: float32 [3, 49152], P(None, ('rep', 'gx')), parts along dimension 1
- new_velocities: float32 [3, 49152], P(None, ('rep', 'gx')), parts along dimension 1
- new_positions: float32 [3, 49152], P(None, ('rep', 'gx')), parts along dimension 1
- new_coupling: float32 [8], P('rep'), parts along dimension 0
The draws below stay inside these ranges and needn't reach their ends.
There are 2 independent parts, one for each index of `rep`. The reference program is written for one: setup_inputs(seed, part) draws one part's arguments, and reference() takes and returns one part's arrays. A program takes and returns all parts, laid end to end along the dimension named above; each array names one. Nothing has to cross between parts.
Inputs may be any that keep to these rules, and one draw needn't show every extreme that they name: `pair_list`: row 0 is a local cluster 0 to 191, row 1 a slot 0 to 479 of the slot table, row 2 an image code 0 to 8. Over each domain's used columns row 0 never falls (the list is grouped by its first cluster). Unused columns hold valid entries too. `pair_count`: at most 16896; some domain uses all 16896 columns in every draw. `exclusion`: each word holds 16 bits; bit 1 means the atom pair interacts. `halo_far`: 96 distinct local clusters of each domain. `atom_params`: rows 1 to 3 are positive.
All inputs are finite; a program needn't handle non-finite values.
Results may differ from the reference program's by a relative error of at most 0.0003.
Values sent between devices are 32-bit elements; how exact they have to be, the bound alone decides.
A program may use at most 64 MiB of HBM per device.

```python
import math
import jax
import jax.numpy as jnp
import numpy as np
from jax import lax

LX = 2
LY = 12
LZ = 8
CAND = 88
ATOMS_DEV = 1536
PAIRS_DEV = 16896
COPY_PARTICLES = 24576
PAIRS = 270336
N_GX = 16


def candidate_offsets():
    result = [(0, 0, 0)]
    for shift_y in range(-2, 3):
        for shift_z in range(-2, 3):
            if shift_y > 0 or (shift_y == 0 and shift_z > 0):
                result.append((0, shift_y, shift_z))
    for shift_x in range(1, 4):
        for shift_y in range(-2, 3):
            for shift_z in range(-2, 3):
                result.append((shift_x, shift_y, shift_z))
    return np.array(result, np.int32)


def upper_words():
    result = []
    for word_place in range(4):
        packed_bits = 0
        for bit_place in range(16):
            number = word_place * 16 + bit_place
            if number % 8 > number // 8:
                packed_bits += 1 << bit_place
        result.append(packed_bits)
    return np.array(result, np.int32)


def cluster_sites(key):
    subkeys = jax.random.split(jax.random.fold_in(key, 101), N_GX)
    return jax.vmap(lambda single: jax.random.permutation(single, LX * LY * LZ))(subkeys).astype(jnp.int32)


def box_stretch(key):
    return jax.random.uniform(jax.random.fold_in(key, 202), (3,), jnp.float32, -0.02, 0.02)


def pair_counts(key):
    base_counts = jax.random.randint(jax.random.fold_in(key, 303), (N_GX,), PAIRS_DEV // 8, PAIRS_DEV // 2 + 1)
    dense_counts = jax.random.randint(jax.random.fold_in(key, 304), (N_GX,), 3 * PAIRS_DEV // 4, PAIRS_DEV + 1)
    dense_start = jax.random.randint(jax.random.fold_in(key, 305), (), 0, N_GX)
    distance = (jnp.arange(N_GX, dtype=jnp.int32) - dense_start) % N_GX
    counts = jnp.where(distance < max(N_GX // 8, 1), dense_counts, base_counts)
    return jnp.where(distance == 0, PAIRS_DEV, counts).astype(jnp.int32)


def pair_order(key):
    counts = pair_counts(key)
    subkeys = jax.random.split(jax.random.fold_in(key, 306), N_GX)
    ranks = jax.vmap(lambda single: jax.random.permutation(single, PAIRS_DEV))(subkeys)
    candidate = jnp.arange(PAIRS_DEV, dtype=jnp.int32)[None, :]
    sort_key = jnp.where(ranks < counts[:, None], candidate, candidate + PAIRS_DEV)
    return jnp.argsort(sort_key, axis=1).astype(jnp.int32)


def pair_tables(key):
    site_of = cluster_sites(key)
    cluster_at = jnp.argsort(site_of, axis=1).astype(jnp.int32)
    plane_size = LY * LZ
    clusters = LX * plane_size
    offsets = jnp.asarray(candidate_offsets())
    layer_x = (site_of // plane_size)[:, :, None]
    layer_y = (site_of // LZ % LY)[:, :, None]
    layer_z = (site_of % LZ)[:, :, None]
    target_x = layer_x + offsets[:, 0]
    raw_y = layer_y + offsets[:, 1]
    raw_z = layer_z + offsets[:, 2]
    wrap_y = (raw_y >= LY).astype(jnp.int32) - (raw_y < 0).astype(jnp.int32)
    wrap_z = (raw_z >= LZ).astype(jnp.int32) - (raw_z < 0).astype(jnp.int32)
    target_y = raw_y - wrap_y * LY
    target_z = raw_z - wrap_z * LZ
    image_code = (wrap_y + 1) * 3 + wrap_z + 1
    in_plane = target_y * LZ + target_z
    own_site = jnp.clip(target_x, 0, LX - 1) * plane_size + in_plane
    near_site = jnp.clip(target_x - LX, 0, LX - 1) * plane_size + in_plane
    next_at = jnp.roll(cluster_at, -1, axis=0)
    own_slot = jnp.take_along_axis(cluster_at, own_site.reshape(N_GX, -1), axis=1).reshape(own_site.shape)
    near_slot = clusters + jnp.take_along_axis(next_at, near_site.reshape(N_GX, -1), axis=1).reshape(near_site.shape)
    far_slot = 2 * clusters + in_plane
    second = jnp.where(target_x < LX, own_slot, jnp.where(target_x < 2 * LX, near_slot, far_slot))
    first = jnp.broadcast_to(jnp.arange(clusters, dtype=jnp.int32)[None, :, None], second.shape)
    is_self = jnp.broadcast_to((jnp.arange(CAND) == 0)[None, None, :], second.shape)
    tables = jnp.stack([first, second, image_code]).reshape(3, N_GX, clusters * CAND).astype(jnp.int32)
    return (tables, is_self.reshape(N_GX, clusters * CAND))


def draw_positions(key, part):
    site_of = cluster_sites(key)
    stretch = box_stretch(key)
    plane_size = LY * LZ
    layer_x = (site_of // plane_size)[:, :, None]
    layer_y = (site_of // LZ % LY)[:, :, None]
    layer_z = (site_of % LZ)[:, :, None]
    atom_slot = jnp.arange(8, dtype=jnp.int32)
    domain = jnp.arange(N_GX, dtype=jnp.int32)[:, None, None]
    coord_x = (domain * LX + layer_x) * 2 + atom_slot // 4
    coord_y = layer_y * 2 + atom_slot // 2 % 2
    coord_z = layer_z * 2 + atom_slot % 2
    lattice = jnp.stack([coord_x, coord_y, coord_z]).astype(jnp.float32).reshape(3, COPY_PARTICLES) + 0.5
    jitter = jax.random.uniform(jax.random.fold_in(key, 203), (3, COPY_PARTICLES), jnp.float32, -0.05, 0.05)
    return lattice * (1.0 + stretch[:, None]) + jitter


def draw_box_lengths(key, part):
    nominal = jnp.array([2.0 * LX * N_GX, 2.0 * LY, 2.0 * LZ], jnp.float32)
    return nominal * (1.0 + box_stretch(key))


def draw_velocities(key, part):
    domain = (jnp.arange(COPY_PARTICLES, dtype=jnp.int32) // ATOMS_DEV).astype(jnp.float32)
    spread = jnp.sqrt(1.0 + 2.0 * domain / (N_GX - 1))
    base = jnp.clip(jax.random.normal(jax.random.fold_in(key, 501), (3, COPY_PARTICLES), jnp.float32), -5.0, 5.0)
    return base * spread[None, :]


def draw_atom_params(key, part):
    charge = jax.random.uniform(jax.random.fold_in(key, 601), (COPY_PARTICLES,), jnp.float32, -1.0, 1.0)
    dispersion = jnp.exp(jax.random.uniform(jax.random.fold_in(key, 602), (COPY_PARTICLES,), jnp.float32, math.log(0.3), 0.0))
    repulsion = jnp.exp(jax.random.uniform(jax.random.fold_in(key, 603), (COPY_PARTICLES,), jnp.float32, math.log(0.1), math.log(0.3)))
    inverse_mass = jnp.exp(jax.random.uniform(jax.random.fold_in(key, 604), (COPY_PARTICLES,), jnp.float32, math.log(0.5), math.log(2.0)))
    return jnp.stack([charge, dispersion, repulsion, inverse_mass])


def draw_pair_list(key, part):
    tables, is_self = pair_tables(key)
    order = pair_order(key)
    return jnp.take_along_axis(tables, order[None, :, :], axis=2).reshape(3, PAIRS)


def draw_pair_count(key, part):
    return pair_counts(key)


def draw_exclusion(key, part):
    tables, is_self = pair_tables(key)
    order = pair_order(key)
    first_words = jax.random.randint(jax.random.fold_in(key, 401), (4, N_GX, PAIRS_DEV), 0, 65536)
    second_words = jax.random.randint(jax.random.fold_in(key, 402), (4, N_GX, PAIRS_DEV), 0, 65536)
    words = first_words | second_words
    upper = jnp.asarray(upper_words())[:, None, None]
    words = jnp.where(is_self[None, :, :], words & upper, words)
    return jnp.take_along_axis(words, order[None, :, :], axis=2).reshape(4, PAIRS).astype(jnp.int32)


def draw_halo_far(key, part):
    site_of = cluster_sites(key)
    cluster_at = jnp.argsort(site_of, axis=1).astype(jnp.int32)
    return cluster_at[:, :LY * LZ].reshape(N_GX * LY * LZ)


def setup_inputs(seed: int = 0, part: int = 0) -> dict:
    seeds = jax.random.split(jax.random.key(seed), 10)
    part_keys = jax.random.split(jax.random.fold_in(seeds[9], part), 10)
    return {
        "positions": draw_positions(jax.random.fold_in(jax.random.fold_in(seeds[9], part), 71), part),
        "velocities": draw_velocities(jax.random.fold_in(jax.random.fold_in(seeds[9], part), 71), part),
        "atom_params": draw_atom_params(jax.random.fold_in(jax.random.fold_in(seeds[9], part), 71), part),
        "pair_list": draw_pair_list(jax.random.fold_in(jax.random.fold_in(seeds[9], part), 71), part),
        "pair_count": draw_pair_count(jax.random.fold_in(jax.random.fold_in(seeds[9], part), 71), part),
        "exclusion": draw_exclusion(jax.random.fold_in(jax.random.fold_in(seeds[9], part), 71), part),
        "halo_far": draw_halo_far(jax.random.fold_in(jax.random.fold_in(seeds[9], part), 71), part),
        "box_lengths": draw_box_lengths(jax.random.fold_in(jax.random.fold_in(seeds[9], part), 71), part),
        "extended_variables": jnp.clip(jax.random.uniform(part_keys[8], (4,), jnp.float32, -0.3, 0.3), -0.3, 0.3),
    }


time_step = 0.25
reaction_term = 1.0 / 1331.0
thermal_scale_unit = 2.0
reservoir_inertia_mass = 4.0
barostat_gain = 0.1
pressure_target = 1.0

def pair_tiles(slot_table, pair_rows, word_rows, usable, box_lengths):
    tile_width = pair_rows.shape[1]
    first_rows = jnp.take(slot_table, pair_rows[0], axis=0).T.reshape(6, 8, tile_width)
    second_rows = jnp.take(slot_table, pair_rows[1], axis=0).T.reshape(6, 8, tile_width)
    image_y = (pair_rows[2] // 3 - 1).astype(jnp.float32) * box_lengths[1]
    image_z = (pair_rows[2] % 3 - 1).astype(jnp.float32) * box_lengths[2]
    delta_x = second_rows[0][None, :, :] - first_rows[0][:, None, :]
    delta_y = second_rows[1][None, :, :] - first_rows[1][:, None, :] + image_y
    delta_z = second_rows[2][None, :, :] - first_rows[2][:, None, :] + image_z
    shifts = (jnp.arange(64, dtype=jnp.int32) % 16)[:, None]
    mask_bits = jnp.right_shift(jnp.repeat(word_rows, 16, axis=0), shifts) & 1
    interact = (mask_bits.reshape(8, 8, tile_width) == 1) & usable[None, None, :]
    radius_sq = delta_x * delta_x + delta_y * delta_y + delta_z * delta_z
    radius_sq = jnp.where(interact, radius_sq, 1.0)
    inverse = lax.rsqrt(radius_sq)
    inverse_sq = inverse * inverse
    inverse_six = inverse_sq * inverse_sq * inverse_sq
    charge_pair = first_rows[3][:, None, :] * second_rows[3][None, :, :]
    dispersion = first_rows[4][:, None, :] * second_rows[4][None, :, :]
    repulsion = first_rows[5][:, None, :] * second_rows[5][None, :, :]
    scalar = charge_pair * (inverse * inverse_sq - reaction_term) + (12.0 * repulsion * inverse_six - 6.0 * dispersion) * inverse_six * inverse_sq
    scalar = jnp.where(interact, scalar, 0.0)
    components = (delta_x, delta_y, delta_z)
    onto_second = jnp.stack([lax.optimization_barrier(jnp.sum(scalar * component, axis=0)) for component in components])
    onto_first = -jnp.stack([lax.optimization_barrier(jnp.sum(scalar * component, axis=1)) for component in components])
    virial = -0.5 * jnp.stack([jnp.sum(scalar * component * component) for component in components])
    tile_terms = jnp.concatenate([onto_first.reshape(24, tile_width), onto_second.reshape(24, tile_width)], axis=1).T
    owners = jnp.concatenate([pair_rows[0], pair_rows[1]])
    return (tile_terms, owners, virial)

def device_forces(slot_table, pair_rows, word_rows, pair_total, box_lengths):
    slots = slot_table.shape[0]
    block_rows = PAIRS_DEV // LY
    starts = jnp.arange(LY, dtype=jnp.int32) * block_rows

    def one_block(running, first_row):
        accumulated, virial = running
        pair_block = lax.dynamic_slice_in_dim(pair_rows, first_row, block_rows, 1)
        word_block = lax.dynamic_slice_in_dim(word_rows, first_row, block_rows, 1)
        usable = first_row + jnp.arange(block_rows, dtype=jnp.int32) < pair_total
        tile_terms, owners, partial_value = pair_tiles(slot_table, pair_block, word_block, usable, box_lengths)
        accumulated = accumulated + jax.ops.segment_sum(tile_terms, owners, num_segments=slots)
        return ((accumulated, virial + partial_value), None)
    start_state = (jnp.zeros((slots, 24), jnp.float32), jnp.zeros((3,), jnp.float32))
    result, unused = lax.scan(one_block, start_state, starts)
    return result

def reference(positions, velocities, atom_params, pair_list, pair_count, exclusion, halo_far, box_lengths, extended_variables):
    clusters = LX * LY * LZ
    far_clusters = LY * LZ
    slots = 2 * clusters + far_clusters
    packed = jnp.concatenate([positions, atom_params[:3]], axis=0)
    packed = packed.reshape(6, N_GX, clusters, 8).transpose(1, 0, 2, 3)
    far_lists = halo_far.reshape(N_GX, far_clusters)
    far_rows = jax.vmap(lambda block_data, chosen: block_data[:, chosen, :])(packed, far_lists)
    domain = jnp.arange(N_GX, dtype=jnp.int32)
    near_rows = jnp.roll(packed, -1, axis=0)
    far_in = jnp.roll(far_rows, -2, axis=0)
    near_lift = jnp.where(domain == N_GX - 1, box_lengths[0], 0.0)
    far_lift = jnp.where(domain >= N_GX - 2, box_lengths[0], 0.0)
    near_rows = near_rows.at[:, 0].add(near_lift[:, None, None])
    far_in = far_in.at[:, 0].add(far_lift[:, None, None])
    tables = jnp.concatenate([packed, near_rows, far_in], axis=2)
    tables = tables.transpose(0, 2, 1, 3).reshape(N_GX, slots, 48)
    pair_blocks = pair_list.reshape(3, N_GX, PAIRS_DEV).transpose(1, 0, 2)
    word_blocks = exclusion.reshape(4, N_GX, PAIRS_DEV).transpose(1, 0, 2)

    def per_domain(item):
        return device_forces(item[0], item[1], item[2], item[3], box_lengths)
    accumulated, virials = lax.map(per_domain, (tables, pair_blocks, word_blocks, pair_count))
    own_part = accumulated[:, :clusters]
    near_back = jnp.roll(accumulated[:, clusters:2 * clusters], 1, axis=0)
    far_back = jnp.roll(accumulated[:, 2 * clusters:], 2, axis=0)
    summed = own_part + near_back
    summed = jax.vmap(lambda block_data, chosen, extra: block_data.at[chosen].add(extra))(summed, far_lists, far_back)
    forces = summed.reshape(N_GX, clusters, 3, 8).transpose(2, 0, 1, 3).reshape(3, COPY_PARTICLES)
    inverse_mass = atom_params[3]
    kinetic = 0.5 * lax.optimization_barrier(jnp.sum(velocities * velocities / inverse_mass[None, :], axis=1))
    virial = lax.optimization_barrier(jnp.sum(virials, axis=0))
    overall_motion_work = jnp.sum(kinetic)
    volume = box_lengths[0] * box_lengths[1] * box_lengths[2]
    thermal_ratio_value = 2.0 * overall_motion_work / (3.0 * COPY_PARTICLES * thermal_scale_unit)
    reservoir_damping = extended_variables[0] + reservoir_inertia_mass * (thermal_ratio_value - 1.0)
    box_rates = extended_variables[1:] + barostat_gain * (kinetic - virial - pressure_target * volume / 2.0) / (overall_motion_work / 3.0)
    new_velocities = velocities + time_step * (forces * inverse_mass[None, :] - (reservoir_damping + box_rates[:, None]) * velocities)
    new_positions = positions * (1.0 + time_step * box_rates[:, None]) + time_step * new_velocities
    new_coupling = jnp.concatenate([reservoir_damping[None], box_rates])
    return (forces, new_velocities, new_positions, new_coupling)
```

```python
import functools

import jax
import jax.numpy as jnp
from jax import lax
from jax.experimental import pallas as pl
from jax.experimental.pallas import tpu as pltpu
from jax.sharding import PartitionSpec as P

time_step = 0.25
reaction_term = 1.0 / 1331.0
thermal_scale_unit = 2.0
reservoir_inertia_mass = 4.0
barostat_gain = 0.1
pressure_target = 1.0

LANES = 128
FAR_AWAY = 1e36


def round_up(value, unit):
    return (value + unit - 1) // unit * unit


def split_two(parts):
    value = jnp.concatenate(parts, axis=0)
    high = value.astype(jnp.bfloat16)
    low = (value - high.astype(jnp.float32)).astype(jnp.bfloat16)
    return jnp.concatenate([high, low], axis=0)


def picked_rows(table_ref, index, first_tile, last_tile, held=None):
    within = index & (LANES - 1)
    block = index // LANES
    result = []
    for component in range(6):
        value = None if held is None else held[component]
        for tile in range(first_tile, last_tile):
            source = table_ref[component * 8 : component * 8 + 8, tile * LANES : (tile + 1) * LANES]
            picked = jnp.take_along_axis(source, within, axis=1, mode="promise_in_bounds")
            value = picked if value is None else jnp.where(block == tile, picked, value)
        result.append(value)
    return result


def step_kernel(
    box_ref, extended_ref, count_ref, position_in, velocity_in, param_in, pair_in, word_in, halo_in,
    force_out, velocity_out, position_out, coupling_out,
    position_ref, velocity_ref, param_ref, pair_ref, word_ref, halo_ref,
    table_ref, packed_ref, near_got, far_send, far_got, near_push, far_push, near_back, far_back,
    sum_ref, all_sums, place_ref, folded_ref,
    first_kept, far_kept, term_kept, first_hot, second_hot,
    second_got, first_terms, second_terms, own_ref, other_ref, virial_ref,
    local_sems, send_sems, recv_sems, give_sems, take_sems,
    *, count, clusters, slots, block
):
    me = lax.axis_index("gx")
    parts = block // LANES
    pairs = pair_ref.shape[1]
    blocks = pairs // block
    far_count = slots - 2 * clusters
    first_tiles = -(-clusters // LANES)
    second_tiles = -(-slots // LANES)
    barrier = pltpu.get_barrier_semaphore()

    def greet(step, carry):
        pl.semaphore_signal(
            barrier, inc=1, device_id={"gx": lax.rem(me + step, count)},
            device_id_type=pl.DeviceIdType.MESH,
        )
        return carry

    lax.fori_loop(1, count, greet, 0)
    inward = [
        pltpu.make_async_copy(source, target, local_sems.at[number])
        for number, (source, target) in enumerate((
            (position_in, position_ref), (param_in, param_ref), (halo_in, halo_ref),
            (pair_in, pair_ref), (word_in, word_ref), (velocity_in, velocity_ref),
        ))
    ]
    for copy in inward:
        copy.start()

    sublane = lax.broadcasted_iota(jnp.int32, (8, LANES), 0)
    lane = lax.broadcasted_iota(jnp.int32, (8, LANES), 1)
    own_ref[...] = jnp.zeros_like(own_ref)
    other_ref[...] = jnp.zeros_like(other_ref)
    virial_ref[...] = jnp.zeros_like(virial_ref)
    first_terms[...] = jnp.zeros_like(first_terms)
    second_terms[...] = jnp.zeros_like(second_terms)
    packed_ref[...] = jnp.zeros_like(packed_ref)
    table_ref[...] = jnp.zeros_like(table_ref)

    for copy in inward[:3]:
        copy.wait()
    place = (lane & 15) * 8 + sublane
    for component in range(6):
        source = position_ref if component < 3 else param_ref
        row = component % 3
        for start in range(0, clusters, LANES):
            width = min(LANES, clusters - start)
            value = jnp.zeros((8, LANES), jnp.float32)
            for piece in range(width // 16):
                at = start * 8 + piece * LANES
                spread = jnp.broadcast_to(source[row : row + 1, at : at + LANES], (8, LANES))
                picked = jnp.take_along_axis(spread, place, axis=1, mode="promise_in_bounds")
                value = jnp.where(lane // 16 == piece, picked, value)
            packed_ref[component * 8 : component * 8 + 8, start : start + LANES] = value
    for start in range(0, far_count, LANES):
        width = min(LANES, far_count - start)
        chosen = halo_ref[0:1, start : start + width]
        if width < LANES:
            chosen = jnp.concatenate([chosen, jnp.zeros((1, LANES - width), jnp.int32)], axis=1)
        values = picked_rows(packed_ref, jnp.broadcast_to(chosen, (8, LANES)), 0, first_tiles)
        for component in range(6):
            far_send[component * 8 : component * 8 + 8, start : start + LANES] = values[component]
    table_ref[:, 0:clusters] = packed_ref[:, 0:clusters]

    def remote(source, target, number, hops):
        return pltpu.make_async_remote_copy(
            src_ref=source, dst_ref=target,
            send_sem=send_sems.at[number], recv_sem=recv_sems.at[number],
            device_id={"gx": lax.rem(me + hops, count)}, device_id_type=pl.DeviceIdType.MESH,
        )

    pl.semaphore_wait(barrier, count - 1)
    outward = [remote(far_send, far_got, 1, count - 2), remote(packed_ref, near_got, 0, count - 1)]
    for copy in outward:
        copy.start()
    for copy in inward[3:]:
        copy.wait()

    total = count_ref[0]
    pair_lane = lax.broadcasted_iota(jnp.int32, (16, LANES), 1)

    def hot(column, width, target, at):
        index = jnp.broadcast_to(column, (LANES, LANES)).astype(jnp.int16)
        for start in range(0, width, LANES):
            wanted = (lax.broadcasted_iota(jnp.int32, (LANES, LANES), 1) + start).astype(jnp.int16)
            target[pl.ds(at, LANES), start : start + LANES] = jnp.where(
                index == wanted, jnp.bfloat16(1), jnp.bfloat16(0)
            )

    def prepare(number, carry):
        rows = []
        for row in range(2):
            for part in range(parts):
                at = pl.multiple_of(number * block + part * LANES, LANES)
                rows.append(pair_ref[row : row + 1, pl.ds(at, LANES)])
        if len(rows) % 8:
            rows.append(jnp.zeros((8 - len(rows) % 8, LANES), jnp.int32))
        columns = jnp.concatenate(rows, axis=0).T
        for part in range(parts):
            at = pl.multiple_of(number * block + part * LANES, LANES)
            here = pl.ds(at, LANES)
            hot(columns[:, part : part + 1], first_hot.shape[1], first_hot, at)
            hot(columns[:, parts + part : parts + part + 1], second_hot.shape[1], second_hot, at)
            first = picked_rows(
                packed_ref, jnp.broadcast_to(pair_ref[0:1, here], (8, LANES)), 0, first_tiles
            )
            for c in range(3):
                origin = first[c][0:1]
                first_kept[48 + c : 49 + c, here] = origin
                first[c] = first[c] - jnp.broadcast_to(origin, (8, LANES))
            first[4] = 6.0 * first[4]
            first[5] = 12.0 * first[5]
            for c in range(6):
                first_kept[c * 8 : c * 8 + 8, here] = first[c]
            words = [jnp.broadcast_to(word_ref[w : w + 1, here], (8, LANES)) for w in range(4)]
            low = jnp.where(sublane < 2, words[0], words[1])
            high = jnp.where(sublane < 6, words[2], words[3])
            bits = jnp.where(sublane < 4, low, high) >> (8 * (sublane & 1))
            bits = jnp.where(at + lane < total, bits, 0)
            for turn in range(8):
                wanted = (bits & (1 << ((sublane + turn) & 7))) != 0
                rows8 = slice(turn * 8, turn * 8 + 8)
                far_kept[rows8, here] = jnp.where(wanted, 0.0, FAR_AWAY)
                term_kept[rows8, here] = jnp.where(wanted, reaction_term, 0.0)
        return carry

    lax.fori_loop(0, blocks, prepare, 0)
    energy = velocity_ref[...] * velocity_ref[...] / param_ref[3:4, :]
    energy = 0.5 * jnp.sum(energy, axis=1, keepdims=True)
    place_ref[...] = jnp.full_like(place_ref, -1)
    for start in range(0, far_count, LANES):
        width = min(LANES, far_count - start)
        chosen = halo_ref[0:1, start : start + width].astype(jnp.float32)
        for base in range(0, clusters, LANES):
            height = min(LANES, clusters - base)
            wanted = lax.broadcasted_iota(jnp.int32, (LANES, width), 0).astype(jnp.float32) + base
            hit = jnp.where(jnp.broadcast_to(chosen, (LANES, width)) == wanted, 1.0, 0.0)
            column = lax.broadcasted_iota(jnp.int32, (8, width), 1).astype(jnp.float32)
            found = lax.dot_general(
                jnp.concatenate([column + 1.0, jnp.zeros((8, width), jnp.float32)], axis=0).astype(jnp.bfloat16),
                hit.astype(jnp.bfloat16), (((1,), (1,)), ((), ())), preferred_element_type=jnp.float32,
            )[0:8].astype(jnp.int32)
            held = place_ref[:, base : base + LANES]
            place_ref[:, base : base + LANES] = jnp.where(found > 0, found - 1 + start, held)

    for copy in outward:
        copy.wait()
    near_lift = jnp.where(me >= count - 1, box_ref[0], 0.0)
    far_lift = jnp.where(me >= count - 2, box_ref[0], 0.0)
    upper = lax.broadcasted_iota(jnp.int32, (48, clusters), 0) < 8
    table_ref[:, clusters : 2 * clusters] = near_got[:, 0:clusters] + jnp.where(upper, near_lift, 0.0)
    upper = lax.broadcasted_iota(jnp.int32, (48, far_count), 0) < 8
    table_ref[:, 2 * clusters : slots] = far_got[:, 0:far_count] + jnp.where(upper, far_lift, 0.0)
    box_y = box_ref[1]
    box_z = box_ref[2]

    def fetch(number, part):
        at = pl.multiple_of(number * block + part * LANES, LANES)
        here = pl.ds(at, LANES)
        lanes = slice(part * LANES, (part + 1) * LANES)
        image = jnp.broadcast_to(pair_ref[2:3, here], (8, LANES))
        second = picked_rows(
            table_ref, jnp.broadcast_to(pair_ref[1:2, here], (8, LANES)), 0, second_tiles
        )
        step_y = jnp.where(image >= 6, 1.0, jnp.where(image >= 3, 0.0, -1.0))
        step_z = image.astype(jnp.float32) - 3.0 * step_y - 4.0
        shift = (None, step_y * box_y, step_z * box_z)
        for c in range(3):
            second[c] = second[c] - jnp.broadcast_to(first_kept[48 + c : 49 + c, here], (8, LANES))
            if shift[c] is not None:
                second[c] = second[c] + shift[c]
        for c in range(6):
            second_got[c * 8 : c * 8 + 8, lanes] = second[c]

    def interact(number, part):
        here = pl.ds(pl.multiple_of(number * block + part * LANES, LANES), LANES)
        lanes = slice(part * LANES, (part + 1) * LANES)
        first = [first_kept[c * 8 : c * 8 + 8, here] for c in range(6)]
        second = [second_got[c * 8 : c * 8 + 8, lanes] for c in range(6)]
        charge, dispersion, repulsion = first[3], first[4], first[5]
        moving = second
        from_first = [None] * 3
        onto_second = [None] * 3
        for turn in range(7, -1, -1):
            moving = [pltpu.roll(m, 1, 0) for m in moving] if turn else second
            delta = [moving[c] - first[c] for c in range(3)]
            rows8 = slice(turn * 8, turn * 8 + 8)
            radius_sq = delta[0] * delta[0] + delta[1] * delta[1] + delta[2] * delta[2]
            inverse = lax.rsqrt(radius_sq + far_kept[rows8, here])
            inverse_sq = inverse * inverse
            cube = inverse * inverse_sq
            six = cube * cube
            scalar = charge * moving[3] * (cube - term_kept[rows8, here]) + (
                repulsion * moving[5] * six - dispersion * moving[4]
            ) * (six * inverse_sq)
            for c in range(3):
                force = scalar * delta[c]
                if from_first[c] is None:
                    from_first[c] = force
                    onto_second[c] = force
                else:
                    from_first[c] = from_first[c] + force
                    onto_second[c] = pltpu.roll(onto_second[c], 1, 0) + force
        first_terms[:, lanes] = split_two(from_first)
        second_terms[:, lanes] = split_two(onto_second)
        return [onto_second[c] * second[c] - from_first[c] * first[c] for c in range(3)]

    def spread(number):
        here = pl.ds(pl.multiple_of(number * block, LANES), block)
        contract = (((1,), (0,)), ((), ()))
        own_ref[...] += lax.dot_general(
            first_terms[...], first_hot[here, :], contract, preferred_element_type=jnp.float32
        )
        other_ref[...] += lax.dot_general(
            second_terms[...], second_hot[here, :], contract, preferred_element_type=jnp.float32
        )

    for part in range(parts):
        fetch(0, part)

    def one_block(number, carry):
        spread(jnp.maximum(number - 1, 0))
        upcoming = jnp.minimum(number + 1, blocks - 1)
        virial = [virial_ref[c * 8 : c * 8 + 8, :] for c in range(3)]
        for part in range(parts):
            added = interact(number, part)
            virial = [virial[c] + added[c] for c in range(3)]
            fetch(upcoming, part)
        for c in range(3):
            virial_ref[c * 8 : c * 8 + 8, :] = virial[c]
        return carry

    lax.fori_loop(0, blocks, one_block, 0)
    spread(blocks - 1)
    rows = [
        jnp.sum(jnp.sum(virial_ref[c * 8 : c * 8 + 8, :], axis=0, keepdims=True), axis=1, keepdims=True) * -0.5
        for c in range(3)
    ]
    rows = rows + [energy, jnp.zeros((2, 1), jnp.float32)]
    sum_ref[...] = jnp.broadcast_to(jnp.concatenate(rows, axis=0), (8, LANES))

    def sum_copy(step, source):
        return pltpu.make_async_remote_copy(
            src_ref=sum_ref, dst_ref=all_sums.at[source],
            send_sem=give_sems.at[step], recv_sem=take_sems.at[source],
            device_id={"gx": lax.rem(me + step, count)}, device_id_type=pl.DeviceIdType.MESH,
        )

    def give(step, carry):
        sum_copy(step, me).start()
        return carry

    def take(step, carry):
        sum_copy(step, lax.rem(me + count - step, count)).wait()
        return carry

    other = other_ref[0:24, :] + other_ref[24:48, :]
    near_push[:, 0:clusters] = other[:, clusters : 2 * clusters]
    far_push[:, 0:far_count] = other[:, 2 * clusters : slots]
    homeward = [remote(far_push, far_back, 3, 2), remote(near_push, near_back, 2, 1)]
    for copy in homeward:
        copy.start()
    lax.fori_loop(1, count, give, 0)
    all_sums[me] = sum_ref[...]
    folded_ref[:, 0:clusters] = (
        other[:, 0:clusters] - own_ref[0:24, 0:clusters] - own_ref[24:48, 0:clusters]
    )
    for copy in homeward:
        copy.wait()
    place = place_ref[...]
    for base in range(0, clusters, LANES):
        lanes = slice(base, base + LANES)
        index = place[:, lanes]
        within = jnp.maximum(index, 0) & (LANES - 1)
        for c in range(3):
            rows8 = slice(c * 8, c * 8 + 8)
            value = folded_ref[rows8, lanes] + near_back[rows8, lanes]
            for tile in range(-(-far_count // LANES)):
                source = far_back[rows8, tile * LANES : (tile + 1) * LANES]
                picked = jnp.take_along_axis(source, within, axis=1, mode="promise_in_bounds")
                mine = (index >= tile * LANES) & (index < (tile + 1) * LANES)
                value = value + jnp.where(mine, picked, 0.0)
            folded_ref[rows8, lanes] = value
    wanted = sublane == (lane & 7)
    for c in range(3):
        for tile in range(clusters * 8 // LANES):
            at = tile * 16
            source = folded_ref[c * 8 : c * 8 + 8, at // LANES * LANES : at // LANES * LANES + LANES]
            picked = jnp.take_along_axis(
                source, at % LANES + lane // 8, axis=1, mode="promise_in_bounds"
            )
            force_out[c : c + 1, tile * LANES : (tile + 1) * LANES] = jnp.sum(
                jnp.where(wanted, picked, 0.0), axis=0, keepdims=True
            )
    lax.fori_loop(1, count, take, 0)
    totals = lax.fori_loop(
        0, count, lambda source, held: held + all_sums[source], jnp.zeros((8, LANES), jnp.float32)
    )
    virial = totals[0:3]
    kinetic = totals[3:6]
    energy = totals[3:4] + totals[4:5] + totals[5:6]
    volume = box_ref[0] * box_ref[1] * box_ref[2]
    ratio = 2.0 * energy / (3.0 * count * clusters * 8 * thermal_scale_unit)
    damping = extended_ref[0] + reservoir_inertia_mass * (ratio - 1.0)
    change = barostat_gain * (kinetic - virial - pressure_target * volume / 2.0) / (energy / 3.0)
    row = damping
    rates = []
    for c in range(3):
        rates.append(extended_ref[1 + c] + change[c : c + 1])
        row = jnp.where(lane[0:1] == c + 1, rates[c], row)
    coupling_out[...] = row[:, 0:4]
    rates = jnp.concatenate(rates, axis=0)[:, 0:1]
    velocity = velocity_ref[...]
    moved = velocity + time_step * (
        force_out[...] * param_ref[3:4, :] - (damping[:, 0:1] + rates) * velocity
    )
    velocity_out[...] = moved
    position_out[...] = position_ref[...] * (1.0 + time_step * rates) + time_step * moved


def on_device(
    positions,
    velocities,
    atom_params,
    pair_list,
    pair_count,
    exclusion,
    halo_far,
    box_lengths,
    extended_variables,
):
    clusters = positions.shape[1] // 8
    far_clusters = halo_far.shape[0]
    slots = 2 * clusters + far_clusters
    pairs = pair_list.shape[1]
    count = lax.axis_size("gx")
    block = next(b for b in (512, 384, 256, 128) if pairs % b == 0)
    wide = round_up(clusters, LANES)
    wide_far = round_up(far_clusters, LANES)
    wide_slots = round_up(slots, LANES)
    vmem = pl.BlockSpec(memory_space=pltpu.VMEM)
    smem = pl.BlockSpec(memory_space=pltpu.SMEM)
    anywhere = pl.BlockSpec(memory_space=pl.ANY)
    shape = jax.ShapeDtypeStruct(positions.shape, jnp.float32)
    f32 = lambda *dims: pltpu.VMEM(dims, jnp.float32)
    halo = halo_far[None, :]
    forces, new_velocities, new_positions, new_coupling = pl.pallas_call(
        functools.partial(step_kernel, count=count, clusters=clusters, slots=slots, block=block),
        name="step_kernel",
        out_shape=(shape,) * 3 + (jax.ShapeDtypeStruct((1, 4), jnp.float32),),
        in_specs=[smem] * 3 + [anywhere] * 6,
        out_specs=(vmem,) * 4,
        scratch_shapes=[
            f32(*positions.shape), f32(*velocities.shape), f32(*atom_params.shape),
            pltpu.VMEM(pair_list.shape, jnp.int32), pltpu.VMEM(exclusion.shape, jnp.int32),
            pltpu.VMEM(halo.shape, jnp.int32),
            f32(48, wide_slots), f32(48, wide), f32(48, wide), f32(48, wide_far), f32(48, wide_far),
            f32(24, wide), f32(24, wide_far), f32(24, wide), f32(24, wide_far),
            f32(8, LANES), f32(count, 8, LANES),
            pltpu.VMEM((8, wide), jnp.int32), f32(24, wide),
            f32(56, pairs), f32(64, pairs), f32(64, pairs),
            pltpu.VMEM((pairs, wide), jnp.bfloat16), pltpu.VMEM((pairs, wide_slots), jnp.bfloat16),
            f32(48, block), pltpu.VMEM((48, block), jnp.bfloat16), pltpu.VMEM((48, block), jnp.bfloat16),
            f32(48, wide), f32(48, wide_slots), f32(24, LANES),
            pltpu.SemaphoreType.DMA((6,)), pltpu.SemaphoreType.DMA((4,)), pltpu.SemaphoreType.DMA((4,)),
            pltpu.SemaphoreType.DMA((count,)), pltpu.SemaphoreType.DMA((count,)),
        ],
        compiler_params=pltpu.CompilerParams(
            collective_id=0, has_side_effects=True, vmem_limit_bytes=60 * 1024 * 1024
        ),
    )(box_lengths, extended_variables, pair_count, positions, velocities, atom_params, pair_list, exclusion, halo)
    return (forces, new_velocities, new_positions, new_coupling.reshape(4))


def solution(mesh):
    spread = P(None, ("rep", "gx"))
    return jax.shard_map(
        on_device,
        mesh=mesh,
        in_specs=(spread,) * 4 + (P(("rep", "gx")), spread, P(("rep", "gx")), P("rep"), P("rep")),
        out_specs=(spread,) * 3 + (P("rep"),),
        check_vma=False,
    )
```

```python
import functools

import jax
import jax.numpy as jnp
from jax import lax
from jax.experimental import pallas as pl
from jax.experimental.pallas import tpu as pltpu
from jax.sharding import PartitionSpec as P

time_step = 0.25
reaction_term = 1.0 / 1331.0
thermal_scale_unit = 2.0
reservoir_inertia_mass = 4.0
barostat_gain = 0.1
pressure_target = 1.0

LANES = 128
LANE_BITS = LANES.bit_length() - 1
FAR_AWAY = 1e36


def round_up(value, unit):
    return (value + unit - 1) // unit * unit


def split_two(value):
    high = value.astype(jnp.bfloat16).astype(jnp.float32)
    return jnp.concatenate([high, value - high], axis=0).astype(jnp.bfloat16)


def picked_rows(table_ref, index, first_tile, last_tile, held=None):
    within = (index & (LANES - 1)).astype(jnp.uint32)
    block = index >> LANE_BITS
    result = []
    for component in range(6):
        value = None if held is None else held[component]
        for tile in range(first_tile, last_tile):
            source = table_ref[component * 8 : component * 8 + 8, tile * LANES : (tile + 1) * LANES]
            picked = jnp.take_along_axis(source, within, axis=1, mode="promise_in_bounds")
            value = picked if value is None else jnp.where(block == tile, picked, value)
        result.append(value)
    return result


def step_kernel(
    box_ref, extended_ref, count_ref, position_in, velocity_in, param_in, pair_in, word_in, halo_in,
    folded_out, rate_out,
    position_ref, velocity_ref, param_ref, pair_ref, word_ref, halo_ref,
    table_ref, packed_ref, near_got, far_send, far_got, near_push, far_push, near_back, far_back,
    sum_ref, all_sums, place_ref, folded_ref,
    first_kept, far_kept, term_kept, first_hot, second_hot,
    second_got, first_terms, second_terms, own_ref, other_ref, virial_ref,
    local_sems, send_sems, recv_sems, give_sems, take_sems,
    *, count, clusters, slots, block
):
    me = lax.axis_index("gx")
    parts = block // LANES
    pairs = pair_ref.shape[1]
    blocks = pairs // block
    far_count = slots - 2 * clusters
    first_tiles = -(-clusters // LANES)
    second_tiles = -(-slots // LANES)
    barrier = pltpu.get_barrier_semaphore()

    def greet(step, carry):
        pl.semaphore_signal(
            barrier, inc=1, device_id={"gx": lax.rem(me + step, count)},
            device_id_type=pl.DeviceIdType.MESH,
        )
        return carry

    lax.fori_loop(1, count, greet, 0)
    inward = [
        pltpu.make_async_copy(source, target, local_sems.at[number])
        for number, (source, target) in enumerate((
            (position_in, position_ref), (param_in, param_ref), (halo_in, halo_ref),
            (pair_in, pair_ref), (word_in, word_ref), (velocity_in, velocity_ref),
        ))
    ]
    for copy in inward:
        copy.start()

    sublane = lax.broadcasted_iota(jnp.int32, (8, LANES), 0)
    lane = lax.broadcasted_iota(jnp.int32, (8, LANES), 1)
    own_ref[...] = jnp.zeros_like(own_ref)
    other_ref[...] = jnp.zeros_like(other_ref)
    virial_ref[...] = jnp.zeros_like(virial_ref)
    first_terms[...] = jnp.zeros_like(first_terms)
    second_terms[...] = jnp.zeros_like(second_terms)
    packed_ref[...] = jnp.zeros_like(packed_ref)
    table_ref[...] = jnp.zeros_like(table_ref)

    for copy in inward[:3]:
        copy.wait()
    place = (lane & 15) * 8 + sublane
    for component in range(6):
        source = position_ref if component < 3 else param_ref
        row = component % 3
        for start in range(0, clusters, LANES):
            width = min(LANES, clusters - start)
            value = jnp.zeros((8, LANES), jnp.float32)
            for piece in range(width // 16):
                at = start * 8 + piece * LANES
                spread = jnp.broadcast_to(source[row : row + 1, at : at + LANES], (8, LANES))
                picked = jnp.take_along_axis(spread, place, axis=1, mode="promise_in_bounds")
                value = jnp.where(lane // 16 == piece, picked, value)
            packed_ref[component * 8 : component * 8 + 8, start : start + LANES] = value
    for start in range(0, far_count, LANES):
        width = min(LANES, far_count - start)
        chosen = halo_ref[0:1, start : start + width]
        if width < LANES:
            chosen = jnp.concatenate([chosen, jnp.zeros((1, LANES - width), jnp.int32)], axis=1)
        values = picked_rows(packed_ref, jnp.broadcast_to(chosen, (8, LANES)), 0, first_tiles)
        for component in range(6):
            far_send[component * 8 : component * 8 + 8, start : start + LANES] = values[component]
    table_ref[:, 0:clusters] = packed_ref[:, 0:clusters]

    def remote(source, target, number, hops):
        return pltpu.make_async_remote_copy(
            src_ref=source, dst_ref=target,
            send_sem=send_sems.at[number], recv_sem=recv_sems.at[number],
            device_id={"gx": lax.rem(me + hops, count)}, device_id_type=pl.DeviceIdType.MESH,
        )

    pl.semaphore_wait(barrier, count - 1)
    outward = [remote(far_send, far_got, 1, count - 2), remote(packed_ref, near_got, 0, count - 1)]
    for copy in outward:
        copy.start()
    for copy in inward[3:]:
        copy.wait()

    total = count_ref[0]

    def tile_rows(at, height, row):
        return pl.ds(pl.multiple_of(at // LANES * height + row, 8), 8)

    ramps = [
        (lax.broadcasted_iota(jnp.int32, (16, LANES), 0) + group).astype(jnp.float32).astype(jnp.bfloat16)
        for group in range(0, LANES, 16)
    ]

    def hot(index, hots, at):
        low = jnp.broadcast_to((index & (LANES - 1)).astype(jnp.float32), (16, LANES)).astype(jnp.bfloat16)
        for group in range(LANES // 16):
            hots[pl.ds(pl.multiple_of(at + group * 16, 16), 16), :] = jnp.where(
                low == ramps[group], jnp.bfloat16(1), jnp.bfloat16(0)
            )

    def prepare(number, carry):
        for part in range(parts):
            at = pl.multiple_of(number * block + part * LANES, LANES)
            here = pl.ds(at, LANES)
            hot(pair_ref[0:1, here], first_hot, at)
            hot(pair_ref[1:2, here], second_hot, at)
            first = picked_rows(
                packed_ref, jnp.broadcast_to(pair_ref[0:1, here], (8, LANES)), 0, first_tiles
            )
            for c in range(3):
                origin = first[c][0:1]
                first_kept[tile_rows(at, 72, 48 + c * 8), :] = jnp.broadcast_to(origin, (8, LANES))
                first[c] = first[c] - jnp.broadcast_to(origin, (8, LANES))
            first[4] = 6.0 * first[4]
            first[5] = 12.0 * first[5]
            for c in range(6):
                first_kept[tile_rows(at, 72, c * 8), :] = first[c]
            words = [jnp.broadcast_to(word_ref[w : w + 1, here], (8, LANES)) for w in range(4)]
            low = jnp.where(sublane < 2, words[0], words[1])
            high = jnp.where(sublane < 6, words[2], words[3])
            bits = jnp.where(sublane < 4, low, high) >> (8 * (sublane & 1))
            bits = jnp.where(at + lane < total, bits, 0)
            for turn in range(8):
                wanted = (bits & (1 << ((sublane + turn) & 7))) != 0
                far_kept[tile_rows(at, 64, turn * 8), :] = jnp.where(wanted, 0.0, FAR_AWAY)
                term_kept[tile_rows(at, 64, turn * 8), :] = jnp.where(wanted, reaction_term, 0.0)
        return carry

    lax.fori_loop(0, blocks, prepare, 0)
    energy = velocity_ref[...] * velocity_ref[...] / param_ref[3:4, :]
    energy = 0.5 * jnp.sum(energy, axis=1, keepdims=True)
    place_ref[...] = jnp.full_like(place_ref, -1)
    for start in range(0, far_count, LANES):
        width = min(LANES, far_count - start)
        chosen = halo_ref[0:1, start : start + width].astype(jnp.float32)
        for base in range(0, clusters, LANES):
            height = min(LANES, clusters - base)
            wanted = lax.broadcasted_iota(jnp.int32, (LANES, width), 0).astype(jnp.float32) + base
            hit = jnp.where(jnp.broadcast_to(chosen, (LANES, width)) == wanted, 1.0, 0.0)
            column = lax.broadcasted_iota(jnp.int32, (8, width), 1).astype(jnp.float32)
            found = lax.dot_general(
                jnp.concatenate([column + 1.0, jnp.zeros((8, width), jnp.float32)], axis=0).astype(jnp.bfloat16),
                hit.astype(jnp.bfloat16), (((1,), (1,)), ((), ())), preferred_element_type=jnp.float32,
            )[0:8].astype(jnp.int32)
            held = place_ref[:, base : base + LANES]
            place_ref[:, base : base + LANES] = jnp.where(found > 0, found - 1 + start, held)

    for copy in outward:
        copy.wait()
    near_lift = jnp.where(me >= count - 1, box_ref[0], 0.0)
    far_lift = jnp.where(me >= count - 2, box_ref[0], 0.0)
    upper = lax.broadcasted_iota(jnp.int32, (48, clusters), 0) < 8
    table_ref[:, clusters : 2 * clusters] = near_got[:, 0:clusters] + jnp.where(upper, near_lift, 0.0)
    upper = lax.broadcasted_iota(jnp.int32, (48, far_count), 0) < 8
    table_ref[:, 2 * clusters : slots] = far_got[:, 0:far_count] + jnp.where(upper, far_lift, 0.0)
    box_y = box_ref[1]
    box_z = box_ref[2]

    def fetch(number, part, slot):
        at = pl.multiple_of(number * block + part * LANES, LANES)
        here = pl.ds(at, LANES)
        image = jnp.broadcast_to(pair_ref[2:3, here], (8, LANES))
        second = picked_rows(
            table_ref, jnp.broadcast_to(pair_ref[1:2, here], (8, LANES)), 0, second_tiles
        )
        step_y = jnp.where(image >= 6, 1.0, jnp.where(image >= 3, 0.0, -1.0))
        step_z = image.astype(jnp.float32) - 3.0 * step_y - 4.0
        shift = (None, step_y * box_y, step_z * box_z)
        for c in range(3):
            second[c] = second[c] - first_kept[tile_rows(at, 72, 48 + c * 8), :]
            if shift[c] is not None:
                second[c] = second[c] + shift[c]
        for c in range(6):
            low = slot * 96 + c * 16
            second_got[low : low + 8, :] = second[c]
            second_got[low + 8 : low + 16, :] = second[c]

    def interact(number, part):
        at = pl.multiple_of(number * block + part * LANES, LANES)
        first = [first_kept[tile_rows(at, 72, c * 8), :] for c in range(6)]
        low = (part % 2) * 96
        charge, dispersion, repulsion = first[3], first[4], first[5]
        from_first = [None] * 3
        onto_second = [None] * 3
        for turn in range(7, -1, -1):
            moving = [second_got[low + c * 16 + turn : low + c * 16 + turn + 8, :] for c in range(6)]
            delta = [moving[c] - first[c] for c in range(3)]
            radius_sq = delta[0] * delta[0] + delta[1] * delta[1] + delta[2] * delta[2]
            inverse = lax.rsqrt(radius_sq + far_kept[tile_rows(at, 64, turn * 8), :])
            inverse_sq = inverse * inverse
            cube = inverse * inverse_sq
            six = cube * cube
            scalar = charge * moving[3] * (cube - term_kept[tile_rows(at, 64, turn * 8), :]) + (
                repulsion * moving[5] * six - dispersion * moving[4]
            ) * (six * inverse_sq)
            for c in range(3):
                force = scalar * delta[c]
                if from_first[c] is None:
                    from_first[c] = force
                    onto_second[c] = force
                else:
                    from_first[c] = from_first[c] + force
                    onto_second[c] = pltpu.roll(onto_second[c], 1, 0) + force
        for c in range(3):
            first_terms[part * 24 + c * 8 : part * 24 + c * 8 + 8, :] = from_first[c]
            second_terms[part * 24 + c * 8 : part * 24 + c * 8 + 8, :] = onto_second[c]
        return [onto_second[c] * moving[c] - from_first[c] * first[c] for c in range(3)]

    def spread(number):
        for target, terms, row, hots, tiles in (
            (own_ref, first_terms, 0, first_hot, first_tiles),
            (other_ref, second_terms, 1, second_hot, second_tiles),
        ):
            rows = []
            columns = []
            for part in range(parts):
                at = pl.multiple_of(number * block + part * LANES, LANES)
                home = jnp.broadcast_to(pair_ref[row : row + 1, pl.ds(at, LANES)] >> LANE_BITS, (16, LANES))
                home = home.astype(jnp.float32).astype(jnp.bfloat16)
                home = jnp.concatenate([home] * 3, axis=0)
                pieces = split_two(terms[part * 24 : part * 24 + 24, :])
                rows.append(jnp.concatenate([
                    jnp.where(home == jnp.bfloat16(tile), pieces, jnp.bfloat16(0)) for tile in range(tiles)
                ], axis=0))
                columns.append(hots[pl.ds(at, LANES), :])
            target[...] += lax.dot_general(
                jnp.concatenate(rows, axis=1), jnp.concatenate(columns, axis=1),
                (((1,), (1,)), ((), ())), preferred_element_type=jnp.float32,
            )

    fetch(0, 0, 0)

    def one_block(number, carry):
        spread(jnp.maximum(number - 1, 0))
        upcoming = jnp.minimum(number + 1, blocks - 1)
        virial = [virial_ref[c * 8 : c * 8 + 8, :] for c in range(3)]
        for part in range(parts):
            if part + 1 < parts:
                fetch(number, part + 1, (part + 1) % 2)
            else:
                fetch(upcoming, 0, 0)
            added = interact(number, part)
            virial = [virial[c] + added[c] for c in range(3)]
        for c in range(3):
            virial_ref[c * 8 : c * 8 + 8, :] = virial[c]
        return carry

    lax.fori_loop(0, blocks, one_block, 0)
    row = jnp.zeros((1, LANES), jnp.float32)
    for c in range(3):
        added = jnp.sum(virial_ref[c * 8 : c * 8 + 8, :], axis=0, keepdims=True)
        row = jnp.where(lane[0:1] == c, jnp.sum(added, axis=1, keepdims=True) * -0.5, row)
        row = jnp.where(lane[0:1] == c + 3, energy[c : c + 1], row)
    sum_ref[...] = row
    spread(blocks - 1)

    def sum_copy(step, source):
        return pltpu.make_async_remote_copy(
            src_ref=sum_ref, dst_ref=all_sums.at[source],
            send_sem=give_sems.at[step], recv_sem=take_sems.at[source],
            device_id={"gx": lax.rem(me + step, count)}, device_id_type=pl.DeviceIdType.MESH,
        )

    def give(step, carry):
        sum_copy(step, me).start()
        return carry

    def take(step, carry):
        sum_copy(step, lax.rem(me + count - step, count)).wait()
        return carry

    def joined(ref, tiles):
        return jnp.concatenate([
            ref[tile * 48 : tile * 48 + 24, :] + ref[tile * 48 + 24 : tile * 48 + 48, :]
            for tile in range(tiles)
        ], axis=1)

    other = joined(other_ref, second_tiles)
    own = joined(own_ref, first_tiles)
    near_push[:, 0:clusters] = other[:, clusters : 2 * clusters]
    far_push[:, 0:far_count] = other[:, 2 * clusters : slots]
    lax.fori_loop(1, count, give, 0)
    homeward = [remote(far_push, far_back, 3, 2), remote(near_push, near_back, 2, 1)]
    for copy in homeward:
        copy.start()
    all_sums[me] = sum_ref[...]
    folded_ref[:, 0:clusters] = other[:, 0:clusters] - own[:, 0:clusters]
    for copy in homeward:
        copy.wait()
    place = place_ref[...]
    for base in range(0, clusters, LANES):
        lanes = slice(base, base + LANES)
        index = place[:, lanes]
        within = (jnp.maximum(index, 0) & (LANES - 1)).astype(jnp.uint32)
        for c in range(3):
            rows8 = slice(c * 8, c * 8 + 8)
            value = folded_ref[rows8, lanes] + near_back[rows8, lanes]
            for tile in range(-(-far_count // LANES)):
                source = far_back[rows8, tile * LANES : (tile + 1) * LANES]
                picked = jnp.take_along_axis(source, within, axis=1, mode="promise_in_bounds")
                mine = (index >= tile * LANES) & (index < (tile + 1) * LANES)
                value = value + jnp.where(mine, picked, 0.0)
            folded_out[rows8, lanes] = value
    lax.fori_loop(1, count, take, 0)
    totals = lax.fori_loop(
        0, count, lambda source, held: held + all_sums[source], jnp.zeros((1, LANES), jnp.float32)
    )
    virial = [jnp.broadcast_to(totals[:, c : c + 1], (1, LANES)) for c in range(3)]
    kinetic = [jnp.broadcast_to(totals[:, c : c + 1], (1, LANES)) for c in range(3, 6)]
    energy = kinetic[0] + kinetic[1] + kinetic[2]
    volume = box_ref[0] * box_ref[1] * box_ref[2]
    ratio = 2.0 * energy / (3.0 * count * clusters * 8 * thermal_scale_unit)
    rate_out[3:4] = extended_ref[0] + reservoir_inertia_mass * (ratio - 1.0)
    for c in range(3):
        change = barostat_gain * (kinetic[c] - virial[c] - pressure_target * volume / 2.0) / (energy / 3.0)
        rate_out[c : c + 1] = extended_ref[1 + c] + change


def final_kernel(
    folded_ref, rate_ref, position_ref, velocity_ref, param_ref,
    force_out, velocity_out, position_out, coupling_out, *, clusters
):
    sublane = lax.broadcasted_iota(jnp.int32, (8, LANES), 0)
    lane = lax.broadcasted_iota(jnp.int32, (8, LANES), 1)
    wanted = sublane == (lane & 7)
    for c in range(3):
        for tile in range(clusters * 8 // LANES):
            at = tile * 16
            source = folded_ref[c * 8 : c * 8 + 8, at // LANES * LANES : at // LANES * LANES + LANES]
            index = (at % LANES + lane // 8).astype(jnp.uint32)
            picked = jnp.take_along_axis(source, index, axis=1, mode="promise_in_bounds")
            force_out[c : c + 1, tile * LANES : (tile + 1) * LANES] = jnp.sum(
                jnp.where(wanted, picked, 0.0), axis=0, keepdims=True
            )
    row = rate_ref[3:4, :]
    for c in range(3):
        row = jnp.where(lane[0:1] == c + 1, rate_ref[c : c + 1, :], row)
    coupling_out[...] = row[:, 0:4]
    rates = rate_ref[0:3, 0:1]
    damping = rate_ref[3:4, 0:1]
    velocity = velocity_ref[...]
    moved = velocity + time_step * (
        force_out[...] * param_ref[3:4, :] - (damping + rates) * velocity
    )
    velocity_out[...] = moved
    position_out[...] = position_ref[...] * (1.0 + time_step * rates) + time_step * moved


def on_device(
    positions,
    velocities,
    atom_params,
    pair_list,
    pair_count,
    exclusion,
    halo_far,
    box_lengths,
    extended_variables,
):
    clusters = positions.shape[1] // 8
    far_clusters = halo_far.shape[0]
    slots = 2 * clusters + far_clusters
    pairs = pair_list.shape[1]
    count = lax.axis_size("gx")
    block = next(b for b in (768, 512, 384, 256, 128) if pairs % b == 0)
    wide = round_up(clusters, LANES)
    wide_far = round_up(far_clusters, LANES)
    wide_slots = round_up(slots, LANES)
    vmem = pl.BlockSpec(memory_space=pltpu.VMEM)
    smem = pl.BlockSpec(memory_space=pltpu.SMEM)
    anywhere = pl.BlockSpec(memory_space=pl.ANY)
    shape = jax.ShapeDtypeStruct(positions.shape, jnp.float32)
    f32 = lambda *dims: pltpu.VMEM(dims, jnp.float32)
    halo = halo_far[None, :]
    folded, rates = pl.pallas_call(
        functools.partial(step_kernel, count=count, clusters=clusters, slots=slots, block=block),
        name="step_kernel",
        out_shape=(
            jax.ShapeDtypeStruct((24, wide), jnp.float32), jax.ShapeDtypeStruct((4, LANES), jnp.float32)
        ),
        in_specs=[smem] * 3 + [anywhere] * 6,
        out_specs=(vmem,) * 2,
        scratch_shapes=[
            f32(*positions.shape), f32(*velocities.shape), f32(*atom_params.shape),
            pltpu.VMEM(pair_list.shape, jnp.int32), pltpu.VMEM(exclusion.shape, jnp.int32),
            pltpu.VMEM(halo.shape, jnp.int32),
            f32(48, wide_slots), f32(48, wide), f32(48, wide), f32(48, wide_far), f32(48, wide_far),
            f32(24, wide), f32(24, wide_far), f32(24, wide), f32(24, wide_far),
            f32(1, LANES), f32(count, 1, LANES),
            pltpu.VMEM((8, wide), jnp.int32), f32(24, wide),
            f32(pairs // LANES * 72, LANES), f32(pairs // LANES * 64, LANES), f32(pairs // LANES * 64, LANES),
pltpu.VMEM((pairs, LANES), jnp.bfloat16), pltpu.VMEM((pairs, LANES), jnp.bfloat16),
            f32(192, LANES), f32(block // LANES * 24, LANES), f32(block // LANES * 24, LANES),
            f32(wide // LANES * 48, LANES), f32(wide_slots // LANES * 48, LANES), f32(24, LANES),
            pltpu.SemaphoreType.DMA((6,)), pltpu.SemaphoreType.DMA((4,)), pltpu.SemaphoreType.DMA((4,)),
            pltpu.SemaphoreType.DMA((count,)), pltpu.SemaphoreType.DMA((count,)),
        ],
        compiler_params=pltpu.CompilerParams(
            collective_id=0, has_side_effects=True, vmem_limit_bytes=60 * 1024 * 1024
        ),
    )(box_lengths, extended_variables, pair_count, positions, velocities, atom_params, pair_list, exclusion, halo)
    forces, new_velocities, new_positions, new_coupling = pl.pallas_call(
        functools.partial(final_kernel, clusters=clusters),
        name="final_kernel",
        out_shape=(shape,) * 3 + (jax.ShapeDtypeStruct((1, 4), jnp.float32),),
        in_specs=[vmem] * 5,
        out_specs=(vmem,) * 4,
    )(folded, rates, positions, velocities, atom_params)
    return (forces, new_velocities, new_positions, new_coupling.reshape(4))


def solution(mesh):
    spread = P(None, ("rep", "gx"))
    return jax.shard_map(
        on_device,
        mesh=mesh,
        in_specs=(spread,) * 4 + (P(("rep", "gx")), spread, P(("rep", "gx")), P("rep"), P("rep")),
        out_specs=(spread,) * 3 + (P("rep"),),
        check_vma=False,
    )
```

```python
import functools

import jax
import jax.numpy as jnp
from jax import lax
from jax.experimental import pallas as pl
from jax.experimental.pallas import tpu as pltpu
from jax.sharding import PartitionSpec as P

time_step = 0.25
reaction_term = 1.0 / 1331.0
thermal_scale_unit = 2.0
reservoir_inertia_mass = 4.0
barostat_gain = 0.1
pressure_target = 1.0

LANES = 128
LANE_BITS = LANES.bit_length() - 1
FAR_AWAY = 1e36


def round_up(value, unit):
    return (value + unit - 1) // unit * unit


def split_two(value):
    high = value.astype(jnp.bfloat16).astype(jnp.float32)
    return jnp.concatenate([high, value - high], axis=0).astype(jnp.bfloat16)


def picked_rows(table_ref, index, first_tile, last_tile, held=None):
    within = (index & (LANES - 1)).astype(jnp.uint32)
    block = index >> LANE_BITS
    result = []
    for component in range(6):
        value = None if held is None else held[component]
        for tile in range(first_tile, last_tile):
            source = table_ref[component * 8 : component * 8 + 8, tile * LANES : (tile + 1) * LANES]
            picked = jnp.take_along_axis(source, within, axis=1, mode="promise_in_bounds")
            value = picked if value is None else jnp.where(block == tile, picked, value)
        result.append(value)
    return result


def step_kernel(
    box_in, extended_in, count_in, position_in, velocity_in, param_in, pair_in, word_in, halo_in,
    folded_out, rate_out, box_ref, extended_ref, count_ref,
    position_ref, velocity_ref, param_ref, pair_ref, word_ref, halo_ref,
    table_ref, packed_ref, near_got, far_send, far_got, near_push, far_push, near_back, far_back,
    sum_ref, all_sums, place_ref, folded_ref,
    first_kept, far_kept, term_kept, first_hot, second_hot,
    second_got, first_terms, second_terms, own_ref, other_ref, virial_ref,
    local_sems, send_sems, recv_sems, give_sems, take_sems,
    *, count, clusters, slots, block
):
    me = lax.axis_index("gx")
    parts = block // LANES
    pairs = pair_ref.shape[1]
    blocks = pairs // block
    far_count = slots - 2 * clusters
    first_tiles = -(-clusters // LANES)
    second_tiles = -(-slots // LANES)
    barrier = pltpu.get_barrier_semaphore()

    def greet(step, carry):
        pl.semaphore_signal(
            barrier, inc=1, device_id={"gx": lax.rem(me + step, count)},
            device_id_type=pl.DeviceIdType.MESH,
        )
        return carry

    close = sorted({1, count - 1, 2, count - 2} - {0, count})
    for step in close:
        greet(step, 0)
    lax.fori_loop(3, count - 2, greet, 0)
    inward = [
        pltpu.make_async_copy(source, target, local_sems.at[number])
        for number, (source, target) in enumerate((
            (position_in, position_ref), (param_in, param_ref), (halo_in, halo_ref),
            (pair_in, pair_ref), (word_in, word_ref), (count_in, count_ref), (box_in, box_ref),
            (velocity_in, velocity_ref), (extended_in, extended_ref),
        ))
    ]
    for copy in inward:
        copy.start()

    sublane = lax.broadcasted_iota(jnp.int32, (8, LANES), 0)
    lane = lax.broadcasted_iota(jnp.int32, (8, LANES), 1)
    own_ref[...] = jnp.zeros_like(own_ref)
    other_ref[...] = jnp.zeros_like(other_ref)
    virial_ref[...] = jnp.zeros_like(virial_ref)
    first_terms[...] = jnp.zeros_like(first_terms)
    second_terms[...] = jnp.zeros_like(second_terms)
    packed_ref[...] = jnp.zeros_like(packed_ref)
    table_ref[...] = jnp.zeros_like(table_ref)

    for copy in inward[:3]:
        copy.wait()
    place = (lane & 15) * 8 + sublane
    for component in range(6):
        source = position_ref if component < 3 else param_ref
        row = component % 3
        for start in range(0, clusters, LANES):
            width = min(LANES, clusters - start)
            value = jnp.zeros((8, LANES), jnp.float32)
            for piece in range(width // 16):
                at = start * 8 + piece * LANES
                spread = jnp.broadcast_to(source[row : row + 1, at : at + LANES], (8, LANES))
                picked = jnp.take_along_axis(spread, place, axis=1, mode="promise_in_bounds")
                value = jnp.where(lane // 16 == piece, picked, value)
            packed_ref[component * 8 : component * 8 + 8, start : start + LANES] = value
    for start in range(0, far_count, LANES):
        width = min(LANES, far_count - start)
        chosen = halo_ref[0:1, start : start + width]
        if width < LANES:
            chosen = jnp.concatenate([chosen, jnp.zeros((1, LANES - width), jnp.int32)], axis=1)
        values = picked_rows(packed_ref, jnp.broadcast_to(chosen, (8, LANES)), 0, first_tiles)
        for component in range(6):
            far_send[component * 8 : component * 8 + 8, start : start + LANES] = values[component]
    table_ref[:, 0:clusters] = packed_ref[:, 0:clusters]

    def remote(source, target, number, hops):
        return pltpu.make_async_remote_copy(
            src_ref=source, dst_ref=target,
            send_sem=send_sems.at[number], recv_sem=recv_sems.at[number],
            device_id={"gx": lax.rem(me + hops, count)}, device_id_type=pl.DeviceIdType.MESH,
        )

    pl.semaphore_wait(barrier, count - 1)
    outward = [remote(far_send, far_got, 1, count - 2), remote(packed_ref, near_got, 0, count - 1)]
    for copy in outward:
        copy.start()
    for copy in inward[3:7]:
        copy.wait()

    total = count_ref[0]
    box_y = box_ref[1]
    box_z = box_ref[2]

    def tile_rows(at, height, row):
        return pl.ds(pl.multiple_of(at // LANES * height + row, 8), 8)

    ramps = [
        (lax.broadcasted_iota(jnp.int32, (16, LANES), 0) + group).astype(jnp.float32).astype(jnp.bfloat16)
        for group in range(0, LANES, 16)
    ]

    def hot(index, hots, at):
        low = jnp.broadcast_to((index & (LANES - 1)).astype(jnp.float32), (16, LANES)).astype(jnp.bfloat16)
        for group in range(LANES // 16):
            hots[pl.ds(pl.multiple_of(at + group * 16, 16), 16), :] = jnp.where(
                low == ramps[group], jnp.bfloat16(1), jnp.bfloat16(0)
            )

    def prepare(number, carry):
        for part in range(parts):
            at = pl.multiple_of(number * block + part * LANES, LANES)
            here = pl.ds(at, LANES)
            hot(pair_ref[0:1, here], first_hot, at)
            hot(pair_ref[1:2, here], second_hot, at)
            first = picked_rows(
                packed_ref, jnp.broadcast_to(pair_ref[0:1, here], (8, LANES)), 0, first_tiles
            )
            for c in range(3):
                origin = first[c][0:1]
                first_kept[tile_rows(at, 88, 48 + c * 8), :] = jnp.broadcast_to(origin, (8, LANES))
                first[c] = first[c] - jnp.broadcast_to(origin, (8, LANES))
            first[4] = 6.0 * first[4]
            first[5] = 12.0 * first[5]
            for c in range(6):
                first_kept[tile_rows(at, 88, c * 8), :] = first[c]
            image = jnp.broadcast_to(pair_ref[2:3, here], (8, LANES))
            step_y = jnp.where(image >= 6, 1.0, jnp.where(image >= 3, 0.0, -1.0))
            step_z = image.astype(jnp.float32) - 3.0 * step_y - 4.0
            first_kept[tile_rows(at, 88, 72), :] = step_y * box_y
            first_kept[tile_rows(at, 88, 80), :] = step_z * box_z
            words = [jnp.broadcast_to(word_ref[w : w + 1, here], (8, LANES)) for w in range(4)]
            low = jnp.where(sublane < 2, words[0], words[1])
            high = jnp.where(sublane < 6, words[2], words[3])
            bits = jnp.where(sublane < 4, low, high) >> (8 * (sublane & 1))
            bits = jnp.where(at + lane < total, bits, 0)
            for turn in range(8):
                wanted = (bits & (1 << ((sublane + turn) & 7))) != 0
                far_kept[tile_rows(at, 64, turn * 8), :] = jnp.where(wanted, 0.0, FAR_AWAY)
                term_kept[tile_rows(at, 64, turn * 8), :] = jnp.where(wanted, reaction_term, 0.0)
        return carry

    lax.fori_loop(0, blocks, prepare, 0)
    for copy in inward[7:]:
        copy.wait()
    energy = velocity_ref[...] * velocity_ref[...] / param_ref[3:4, :]
    energy = 0.5 * jnp.sum(energy, axis=1, keepdims=True)
    place_ref[...] = jnp.full_like(place_ref, -1)
    for start in range(0, far_count, LANES):
        width = min(LANES, far_count - start)
        chosen = halo_ref[0:1, start : start + width].astype(jnp.float32)
        for base in range(0, clusters, LANES):
            height = min(LANES, clusters - base)
            wanted = lax.broadcasted_iota(jnp.int32, (LANES, width), 0).astype(jnp.float32) + base
            hit = jnp.where(jnp.broadcast_to(chosen, (LANES, width)) == wanted, 1.0, 0.0)
            column = lax.broadcasted_iota(jnp.int32, (8, width), 1).astype(jnp.float32)
            found = lax.dot_general(
                jnp.concatenate([column + 1.0, jnp.zeros((8, width), jnp.float32)], axis=0).astype(jnp.bfloat16),
                hit.astype(jnp.bfloat16), (((1,), (1,)), ((), ())), preferred_element_type=jnp.float32,
            )[0:8].astype(jnp.int32)
            held = place_ref[:, base : base + LANES]
            place_ref[:, base : base + LANES] = jnp.where(found > 0, found - 1 + start, held)

    for copy in outward:
        copy.wait()
    near_lift = jnp.where(me >= count - 1, box_ref[0], 0.0)
    far_lift = jnp.where(me >= count - 2, box_ref[0], 0.0)
    upper = lax.broadcasted_iota(jnp.int32, (48, clusters), 0) < 8
    table_ref[:, clusters : 2 * clusters] = near_got[:, 0:clusters] + jnp.where(upper, near_lift, 0.0)
    upper = lax.broadcasted_iota(jnp.int32, (48, far_count), 0) < 8
    table_ref[:, 2 * clusters : slots] = far_got[:, 0:far_count] + jnp.where(upper, far_lift, 0.0)

    def fetch(number, part, slot):
        at = pl.multiple_of(number * block + part * LANES, LANES)
        here = pl.ds(at, LANES)
        second = picked_rows(
            table_ref, jnp.broadcast_to(pair_ref[1:2, here], (8, LANES)), 0, second_tiles
        )
        for c in range(3):
            second[c] = second[c] - first_kept[tile_rows(at, 88, 48 + c * 8), :]
            if c:
                second[c] = second[c] + first_kept[tile_rows(at, 88, 64 + c * 8), :]
        for c in range(6):
            second_got[slot * 48 + c * 8 : slot * 48 + c * 8 + 8, :] = second[c]

    def interact(number, part):
        at = pl.multiple_of(number * block + part * LANES, LANES)
        first = [first_kept[tile_rows(at, 88, c * 8), :] for c in range(6)]
        low = (part % 2) * 48
        charge, dispersion, repulsion = first[3], first[4], first[5]
        from_first = [None] * 3
        onto_second = [None] * 3
        for turn in range(7, -1, -1):
            moving = [second_got[low + c * 8 : low + c * 8 + 8, :] for c in range(6)]
            if turn:
                moving = [pltpu.roll(m, 8 - turn, 0) for m in moving]
            delta = [moving[c] - first[c] for c in range(3)]
            radius_sq = delta[0] * delta[0] + delta[1] * delta[1] + delta[2] * delta[2]
            inverse = lax.rsqrt(radius_sq + far_kept[tile_rows(at, 64, turn * 8), :])
            inverse_sq = inverse * inverse
            cube = inverse * inverse_sq
            six = cube * cube
            scalar = charge * moving[3] * (cube - term_kept[tile_rows(at, 64, turn * 8), :]) + (
                repulsion * moving[5] * six - dispersion * moving[4]
            ) * (six * inverse_sq)
            for c in range(3):
                force = scalar * delta[c]
                if from_first[c] is None:
                    from_first[c] = force
                    onto_second[c] = force
                else:
                    from_first[c] = from_first[c] + force
                    onto_second[c] = pltpu.roll(onto_second[c], 1, 0) + force
        for c in range(3):
            first_terms[part * 24 + c * 8 : part * 24 + c * 8 + 8, :] = from_first[c]
            second_terms[part * 24 + c * 8 : part * 24 + c * 8 + 8, :] = onto_second[c]
        return [onto_second[c] * moving[c] - from_first[c] * first[c] for c in range(3)]

    def spread(number):
        for target, terms, row, hots, tiles in (
            (own_ref, first_terms, 0, first_hot, first_tiles),
            (other_ref, second_terms, 1, second_hot, second_tiles),
        ):
            rows = []
            columns = []
            for part in range(parts):
                at = pl.multiple_of(number * block + part * LANES, LANES)
                home = jnp.broadcast_to(pair_ref[row : row + 1, pl.ds(at, LANES)] >> LANE_BITS, (16, LANES))
                home = home.astype(jnp.float32).astype(jnp.bfloat16)
                home = jnp.concatenate([home] * 3, axis=0)
                pieces = split_two(terms[part * 24 : part * 24 + 24, :])
                rows.append(jnp.concatenate([
                    jnp.where(home == jnp.bfloat16(tile), pieces, jnp.bfloat16(0)) for tile in range(tiles)
                ], axis=0))
                columns.append(hots[pl.ds(at, LANES), :])
            target[...] += lax.dot_general(
                jnp.concatenate(rows, axis=1), jnp.concatenate(columns, axis=1),
                (((1,), (1,)), ((), ())), preferred_element_type=jnp.float32,
            )

    fetch(0, 0, 0)

    def one_block(number, carry):
        spread(jnp.maximum(number - 1, 0))
        upcoming = jnp.minimum(number + 1, blocks - 1)
        virial = [virial_ref[c * 8 : c * 8 + 8, :] for c in range(3)]
        for part in range(parts):
            if part + 1 < parts:
                fetch(number, part + 1, (part + 1) % 2)
            else:
                fetch(upcoming, 0, 0)
            added = interact(number, part)
            virial = [virial[c] + added[c] for c in range(3)]
        for c in range(3):
            virial_ref[c * 8 : c * 8 + 8, :] = virial[c]
        return carry

    lax.fori_loop(0, blocks, one_block, 0)
    row = jnp.zeros((1, LANES), jnp.float32)
    for c in range(3):
        added = jnp.sum(virial_ref[c * 8 : c * 8 + 8, :], axis=0, keepdims=True)
        row = jnp.where(lane[0:1] == c, jnp.sum(added, axis=1, keepdims=True) * -0.5, row)
        row = jnp.where(lane[0:1] == c + 3, energy[c : c + 1], row)
    sum_ref[...] = row
    spread(blocks - 1)

    def sum_copy(step, source):
        return pltpu.make_async_remote_copy(
            src_ref=sum_ref, dst_ref=all_sums.at[source],
            send_sem=give_sems.at[step], recv_sem=take_sems.at[source],
            device_id={"gx": lax.rem(me + step, count)}, device_id_type=pl.DeviceIdType.MESH,
        )

    def give(step, carry):
        sum_copy(step, me).start()
        return carry

    def take(step, carry):
        sum_copy(step, lax.rem(me + count - step, count)).wait()
        return carry

    def joined(ref, tiles):
        return jnp.concatenate([
            ref[tile * 48 : tile * 48 + 24, :] + ref[tile * 48 + 24 : tile * 48 + 48, :]
            for tile in range(tiles)
        ], axis=1)

    other = joined(other_ref, second_tiles)
    own = joined(own_ref, first_tiles)
    near_push[:, 0:clusters] = other[:, clusters : 2 * clusters]
    far_push[:, 0:far_count] = other[:, 2 * clusters : slots]
    homeward = [remote(far_push, far_back, 3, 2), remote(near_push, near_back, 2, 1)]
    for copy in homeward:
        copy.start()
    lax.fori_loop(1, count, give, 0)
    all_sums[me] = sum_ref[...]
    folded_ref[:, 0:clusters] = other[:, 0:clusters] - own[:, 0:clusters]
    for copy in homeward:
        copy.wait()
    place = place_ref[...]
    for base in range(0, clusters, LANES):
        lanes = slice(base, base + LANES)
        index = place[:, lanes]
        within = (jnp.maximum(index, 0) & (LANES - 1)).astype(jnp.uint32)
        for c in range(3):
            rows8 = slice(c * 8, c * 8 + 8)
            value = folded_ref[rows8, lanes] + near_back[rows8, lanes]
            for tile in range(-(-far_count // LANES)):
                source = far_back[rows8, tile * LANES : (tile + 1) * LANES]
                picked = jnp.take_along_axis(source, within, axis=1, mode="promise_in_bounds")
                mine = (index >= tile * LANES) & (index < (tile + 1) * LANES)
                value = value + jnp.where(mine, picked, 0.0)
            folded_out[rows8, lanes] = value
    lax.fori_loop(1, count, take, 0)
    totals = lax.fori_loop(
        0, count, lambda source, held: held + all_sums[source], jnp.zeros((1, LANES), jnp.float32)
    )
    virial = [jnp.broadcast_to(totals[:, c : c + 1], (1, LANES)) for c in range(3)]
    kinetic = [jnp.broadcast_to(totals[:, c : c + 1], (1, LANES)) for c in range(3, 6)]
    energy = kinetic[0] + kinetic[1] + kinetic[2]
    volume = box_ref[0] * box_ref[1] * box_ref[2]
    ratio = 2.0 * energy / (3.0 * count * clusters * 8 * thermal_scale_unit)
    rate_out[3:4] = extended_ref[0] + reservoir_inertia_mass * (ratio - 1.0)
    for c in range(3):
        change = barostat_gain * (kinetic[c] - virial[c] - pressure_target * volume / 2.0) / (energy / 3.0)
        rate_out[c : c + 1] = extended_ref[1 + c] + change


def final_kernel(
    folded_ref, rate_ref, position_ref, velocity_ref, param_ref,
    force_out, velocity_out, position_out, coupling_out, *, clusters
):
    sublane = lax.broadcasted_iota(jnp.int32, (8, LANES), 0)
    lane = lax.broadcasted_iota(jnp.int32, (8, LANES), 1)
    wanted = sublane == (lane & 7)
    for c in range(3):
        for tile in range(clusters * 8 // LANES):
            at = tile * 16
            source = folded_ref[c * 8 : c * 8 + 8, at // LANES * LANES : at // LANES * LANES + LANES]
            index = (at % LANES + lane // 8).astype(jnp.uint32)
            picked = jnp.take_along_axis(source, index, axis=1, mode="promise_in_bounds")
            force_out[c : c + 1, tile * LANES : (tile + 1) * LANES] = jnp.sum(
                jnp.where(wanted, picked, 0.0), axis=0, keepdims=True
            )
    row = rate_ref[3:4, :]
    for c in range(3):
        row = jnp.where(lane[0:1] == c + 1, rate_ref[c : c + 1, :], row)
    coupling_out[...] = row[:, 0:4]
    rates = rate_ref[0:3, 0:1]
    damping = rate_ref[3:4, 0:1]
    velocity = velocity_ref[...]
    moved = velocity + time_step * (
        force_out[...] * param_ref[3:4, :] - (damping + rates) * velocity
    )
    velocity_out[...] = moved
    position_out[...] = position_ref[...] * (1.0 + time_step * rates) + time_step * moved


def on_device(
    positions,
    velocities,
    atom_params,
    pair_list,
    pair_count,
    exclusion,
    halo_far,
    box_lengths,
    extended_variables,
):
    clusters = positions.shape[1] // 8
    far_clusters = halo_far.shape[0]
    slots = 2 * clusters + far_clusters
    pairs = pair_list.shape[1]
    count = lax.axis_size("gx")
    block = next(b for b in (768, 512, 384, 256, 128) if pairs % b == 0)
    wide = round_up(clusters, LANES)
    wide_far = round_up(far_clusters, LANES)
    wide_slots = round_up(slots, LANES)
    vmem = pl.BlockSpec(memory_space=pltpu.VMEM)
    anywhere = pl.BlockSpec(memory_space=pl.ANY)
    shape = jax.ShapeDtypeStruct(positions.shape, jnp.float32)
    f32 = lambda *dims: pltpu.VMEM(dims, jnp.float32)
    halo = halo_far[None, :]
    folded, rates = pl.pallas_call(
        functools.partial(step_kernel, count=count, clusters=clusters, slots=slots, block=block),
        name="step_kernel",
        out_shape=(
            jax.ShapeDtypeStruct((24, wide), jnp.float32), jax.ShapeDtypeStruct((4, LANES), jnp.float32)
        ),
        in_specs=[anywhere] * 9,
        out_specs=(vmem,) * 2,
        scratch_shapes=[
            pltpu.SMEM(box_lengths.shape, jnp.float32), pltpu.SMEM(extended_variables.shape, jnp.float32),
            pltpu.SMEM(pair_count.shape, jnp.int32),
            f32(*positions.shape), f32(*velocities.shape), f32(*atom_params.shape),
            pltpu.VMEM(pair_list.shape, jnp.int32), pltpu.VMEM(exclusion.shape, jnp.int32),
            pltpu.VMEM(halo.shape, jnp.int32),
            f32(48, wide_slots), f32(48, wide), f32(48, wide), f32(48, wide_far), f32(48, wide_far),
            f32(24, wide), f32(24, wide_far), f32(24, wide), f32(24, wide_far),
            f32(1, LANES), f32(count, 1, LANES),
            pltpu.VMEM((8, wide), jnp.int32), f32(24, wide),
            f32(pairs // LANES * 88, LANES), f32(pairs // LANES * 64, LANES), f32(pairs // LANES * 64, LANES),
pltpu.VMEM((pairs, LANES), jnp.bfloat16), pltpu.VMEM((pairs, LANES), jnp.bfloat16),
            f32(96, LANES), f32(block // LANES * 24, LANES), f32(block // LANES * 24, LANES),
            f32(wide // LANES * 48, LANES), f32(wide_slots // LANES * 48, LANES), f32(24, LANES),
            pltpu.SemaphoreType.DMA((9,)), pltpu.SemaphoreType.DMA((4,)), pltpu.SemaphoreType.DMA((4,)),
            pltpu.SemaphoreType.DMA((count,)), pltpu.SemaphoreType.DMA((count,)),
        ],
        compiler_params=pltpu.CompilerParams(
            collective_id=0, has_side_effects=True, vmem_limit_bytes=60 * 1024 * 1024
        ),
    )(box_lengths, extended_variables, pair_count, positions, velocities, atom_params, pair_list, exclusion, halo)
    forces, new_velocities, new_positions, new_coupling = pl.pallas_call(
        functools.partial(final_kernel, clusters=clusters),
        name="final_kernel",
        out_shape=(shape,) * 3 + (jax.ShapeDtypeStruct((1, 4), jnp.float32),),
        in_specs=[vmem] * 5,
        out_specs=(vmem,) * 4,
    )(folded, rates, positions, velocities, atom_params)
    return (forces, new_velocities, new_positions, new_coupling.reshape(4))


def solution(mesh):
    spread = P(None, ("rep", "gx"))
    return jax.shard_map(
        on_device,
        mesh=mesh,
        in_specs=(spread,) * 4 + (P(("rep", "gx")), spread, P(("rep", "gx")), P("rep"), P("rep")),
        out_specs=(spread,) * 3 + (P("rep"),),
        check_vma=False,
    )
```

```python
import functools

import jax
import jax.numpy as jnp
from jax import lax
from jax.experimental import pallas as pl
from jax.experimental.pallas import tpu as pltpu
from jax.sharding import PartitionSpec as P

time_step = 0.25
reaction_term = 1.0 / 1331.0
thermal_scale_unit = 2.0
reservoir_inertia_mass = 4.0
barostat_gain = 0.1
pressure_target = 1.0

LANES = 128
LANE_BITS = LANES.bit_length() - 1
FAR_AWAY = 1e36


def round_up(value, unit):
    return (value + unit - 1) // unit * unit


def split_two(value):
    high = value.astype(jnp.bfloat16).astype(jnp.float32)
    return jnp.concatenate([high, value - high], axis=0).astype(jnp.bfloat16)


def picked_rows(table_ref, index, first_tile, last_tile, held=None):
    within = (index & (LANES - 1)).astype(jnp.uint32)
    block = index >> LANE_BITS
    result = []
    for component in range(6):
        value = None if held is None else held[component]
        for tile in range(first_tile, last_tile):
            source = table_ref[component * 8 : component * 8 + 8, tile * LANES : (tile + 1) * LANES]
            picked = jnp.take_along_axis(source, within, axis=1, mode="promise_in_bounds")
            value = picked if value is None else jnp.where(block == tile, picked, value)
        result.append(value)
    return result


def step_kernel(
    box_in, extended_in, count_in, position_in, velocity_in, param_in, pair_in, word_in, halo_in,
    folded_out, rate_out, box_ref, extended_ref, count_ref,
    position_ref, velocity_ref, param_ref, pair_ref, word_ref, halo_ref,
    table_ref, packed_ref, near_got, far_send, far_got, near_push, far_push, near_back, far_back,
    sum_ref, all_sums, place_ref, folded_ref,
    first_kept, far_kept, term_kept, first_hot, second_hot,
    second_got, first_terms, second_terms, own_ref, other_ref, virial_ref,
    local_sems, send_sems, recv_sems, give_sems, take_sems,
    *, count, clusters, slots, block
):
    me = lax.axis_index("gx")
    parts = block // LANES
    pairs = pair_ref.shape[1]
    blocks = pairs // block
    far_count = slots - 2 * clusters
    first_tiles = -(-clusters // LANES)
    second_tiles = -(-slots // LANES)
    barrier = pltpu.get_barrier_semaphore()

    def greet(step, carry):
        pl.semaphore_signal(
            barrier, inc=1, device_id={"gx": lax.rem(me + step, count)},
            device_id_type=pl.DeviceIdType.MESH,
        )
        return carry

    close = sorted({1, count - 1, 2, count - 2} - {0, count})
    for step in close:
        greet(step, 0)
    lax.fori_loop(3, count - 2, greet, 0)
    inward = [
        pltpu.make_async_copy(source, target, local_sems.at[number])
        for number, (source, target) in enumerate((
            (position_in, position_ref), (param_in, param_ref), (halo_in, halo_ref),
            (pair_in, pair_ref), (word_in, word_ref), (count_in, count_ref), (box_in, box_ref),
            (velocity_in, velocity_ref), (extended_in, extended_ref),
        ))
    ]
    for copy in inward:
        copy.start()

    sublane = lax.broadcasted_iota(jnp.int32, (8, LANES), 0)
    lane = lax.broadcasted_iota(jnp.int32, (8, LANES), 1)
    own_ref[...] = jnp.zeros_like(own_ref)
    other_ref[...] = jnp.zeros_like(other_ref)
    virial_ref[...] = jnp.zeros_like(virial_ref)
    first_terms[...] = jnp.zeros_like(first_terms)
    second_terms[...] = jnp.zeros_like(second_terms)
    packed_ref[...] = jnp.zeros_like(packed_ref)
    table_ref[...] = jnp.zeros_like(table_ref)

    for copy in inward[:3]:
        copy.wait()
    place = (lane & 15) * 8 + sublane
    for component in range(6):
        source = position_ref if component < 3 else param_ref
        row = component % 3
        for start in range(0, clusters, LANES):
            width = min(LANES, clusters - start)
            value = jnp.zeros((8, LANES), jnp.float32)
            for piece in range(width // 16):
                at = start * 8 + piece * LANES
                spread = jnp.broadcast_to(source[row : row + 1, at : at + LANES], (8, LANES))
                picked = jnp.take_along_axis(spread, place, axis=1, mode="promise_in_bounds")
                value = jnp.where(lane // 16 == piece, picked, value)
            packed_ref[component * 8 : component * 8 + 8, start : start + LANES] = value
    for start in range(0, far_count, LANES):
        width = min(LANES, far_count - start)
        chosen = halo_ref[0:1, start : start + width]
        if width < LANES:
            chosen = jnp.concatenate([chosen, jnp.zeros((1, LANES - width), jnp.int32)], axis=1)
        values = picked_rows(packed_ref, jnp.broadcast_to(chosen, (8, LANES)), 0, first_tiles)
        for component in range(6):
            far_send[component * 8 : component * 8 + 8, start : start + LANES] = values[component]
    table_ref[:, 0:clusters] = packed_ref[:, 0:clusters]

    def remote(source, target, number, hops):
        return pltpu.make_async_remote_copy(
            src_ref=source, dst_ref=target,
            send_sem=send_sems.at[number], recv_sem=recv_sems.at[number],
            device_id={"gx": lax.rem(me + hops, count)}, device_id_type=pl.DeviceIdType.MESH,
        )

    pl.semaphore_wait(barrier, count - 1)
    outward = [remote(far_send, far_got, 1, count - 2), remote(packed_ref, near_got, 0, count - 1)]
    for copy in outward:
        copy.start()
    for copy in inward[3:7]:
        copy.wait()

    total = count_ref[0]
    box_y = box_ref[1]
    box_z = box_ref[2]

    def tile_rows(at, height, row):
        return pl.ds(pl.multiple_of(at // LANES * height + row, 8), 8)

    ramps = [
        (lax.broadcasted_iota(jnp.int32, (16, LANES), 0) + group).astype(jnp.float32).astype(jnp.bfloat16)
        for group in range(0, LANES, 16)
    ]

    def hot(index, hots, at):
        low = jnp.broadcast_to((index & (LANES - 1)).astype(jnp.float32), (16, LANES)).astype(jnp.bfloat16)
        for group in range(LANES // 16):
            hots[pl.ds(pl.multiple_of(at + group * 16, 16), 16), :] = jnp.where(
                low == ramps[group], jnp.bfloat16(1), jnp.bfloat16(0)
            )

    def prepare(number, carry):
        for part in range(parts):
            at = pl.multiple_of(number * block + part * LANES, LANES)
            here = pl.ds(at, LANES)
            hot(pair_ref[0:1, here], first_hot, at)
            hot(pair_ref[1:2, here], second_hot, at)
            first = picked_rows(
                packed_ref, jnp.broadcast_to(pair_ref[0:1, here], (8, LANES)), 0, first_tiles
            )
            for c in range(3):
                origin = first[c][0:1]
                first_kept[tile_rows(at, 88, 48 + c * 8), :] = jnp.broadcast_to(origin, (8, LANES))
                first[c] = first[c] - jnp.broadcast_to(origin, (8, LANES))
            first[4] = 6.0 * first[4]
            first[5] = 12.0 * first[5]
            for c in range(6):
                first_kept[tile_rows(at, 88, c * 8), :] = first[c]
            image = jnp.broadcast_to(pair_ref[2:3, here], (8, LANES))
            step_y = jnp.where(image >= 6, 1.0, jnp.where(image >= 3, 0.0, -1.0))
            step_z = image.astype(jnp.float32) - 3.0 * step_y - 4.0
            first_kept[tile_rows(at, 88, 72), :] = step_y * box_y
            first_kept[tile_rows(at, 88, 80), :] = step_z * box_z
            words = [jnp.broadcast_to(word_ref[w : w + 1, here], (8, LANES)) for w in range(4)]
            low = jnp.where(sublane < 2, words[0], words[1])
            high = jnp.where(sublane < 6, words[2], words[3])
            bits = jnp.where(sublane < 4, low, high) >> (8 * (sublane & 1))
            bits = jnp.where(at + lane < total, bits, 0)
            for turn in range(8):
                wanted = (bits & (1 << ((sublane + turn) & 7))) != 0
                far_kept[tile_rows(at, 64, turn * 8), :] = jnp.where(wanted, 0.0, FAR_AWAY)
                term_kept[tile_rows(at, 64, turn * 8), :] = jnp.where(wanted, reaction_term, 0.0)
        return carry

    lax.fori_loop(0, blocks, prepare, 0)
    for copy in inward[7:]:
        copy.wait()
    energy = velocity_ref[...] * velocity_ref[...] / param_ref[3:4, :]
    energy = 0.5 * jnp.sum(energy, axis=1, keepdims=True)
    place_ref[...] = jnp.full_like(place_ref, -1)
    for start in range(0, far_count, LANES):
        width = min(LANES, far_count - start)
        chosen = halo_ref[0:1, start : start + width].astype(jnp.float32)
        for base in range(0, clusters, LANES):
            height = min(LANES, clusters - base)
            wanted = lax.broadcasted_iota(jnp.int32, (LANES, width), 0).astype(jnp.float32) + base
            hit = jnp.where(jnp.broadcast_to(chosen, (LANES, width)) == wanted, 1.0, 0.0)
            column = lax.broadcasted_iota(jnp.int32, (8, width), 1).astype(jnp.float32)
            found = lax.dot_general(
                jnp.concatenate([column + 1.0, jnp.zeros((8, width), jnp.float32)], axis=0).astype(jnp.bfloat16),
                hit.astype(jnp.bfloat16), (((1,), (1,)), ((), ())), preferred_element_type=jnp.float32,
            )[0:8].astype(jnp.int32)
            held = place_ref[:, base : base + LANES]
            place_ref[:, base : base + LANES] = jnp.where(found > 0, found - 1 + start, held)

    for copy in outward:
        copy.wait()
    near_lift = jnp.where(me >= count - 1, box_ref[0], 0.0)
    far_lift = jnp.where(me >= count - 2, box_ref[0], 0.0)
    upper = lax.broadcasted_iota(jnp.int32, (48, clusters), 0) < 8
    table_ref[:, clusters : 2 * clusters] = near_got[:, 0:clusters] + jnp.where(upper, near_lift, 0.0)
    upper = lax.broadcasted_iota(jnp.int32, (48, far_count), 0) < 8
    table_ref[:, 2 * clusters : slots] = far_got[:, 0:far_count] + jnp.where(upper, far_lift, 0.0)

    def fetch(number, part, slot):
        at = pl.multiple_of(number * block + part * LANES, LANES)
        here = pl.ds(at, LANES)
        second = picked_rows(
            table_ref, jnp.broadcast_to(pair_ref[1:2, here], (8, LANES)), 0, second_tiles
        )
        for c in range(3):
            second[c] = second[c] - first_kept[tile_rows(at, 88, 48 + c * 8), :]
            if c:
                second[c] = second[c] + first_kept[tile_rows(at, 88, 64 + c * 8), :]
        for c in range(6):
            second_got[slot * 48 + c * 8 : slot * 48 + c * 8 + 8, :] = second[c]

    def interact(number, part):
        at = pl.multiple_of(number * block + part * LANES, LANES)
        first = [first_kept[tile_rows(at, 88, c * 8), :] for c in range(6)]
        low = (part % 2) * 48
        charge, dispersion, repulsion = first[3], first[4], first[5]
        from_first = [None] * 3
        onto_second = [None] * 3
        for turn in range(7, -1, -1):
            moving = [second_got[low + c * 8 : low + c * 8 + 8, :] for c in range(6)]
            if turn:
                moving = [pltpu.roll(m, 8 - turn, 0) for m in moving]
            delta = [moving[c] - first[c] for c in range(3)]
            radius_sq = delta[0] * delta[0] + delta[1] * delta[1] + delta[2] * delta[2]
            inverse = lax.rsqrt(radius_sq + far_kept[tile_rows(at, 64, turn * 8), :])
            inverse_sq = inverse * inverse
            cube = inverse * inverse_sq
            six = cube * cube
            scalar = charge * moving[3] * (cube - term_kept[tile_rows(at, 64, turn * 8), :]) + (
                repulsion * moving[5] * six - dispersion * moving[4]
            ) * (six * inverse_sq)
            for c in range(3):
                force = scalar * delta[c]
                if from_first[c] is None:
                    from_first[c] = force
                    onto_second[c] = force
                else:
                    from_first[c] = from_first[c] + force
                    onto_second[c] = pltpu.roll(onto_second[c], 1, 0) + force
        for c in range(3):
            first_terms[part * 24 + c * 8 : part * 24 + c * 8 + 8, :] = from_first[c]
            second_terms[part * 24 + c * 8 : part * 24 + c * 8 + 8, :] = onto_second[c]
        return [onto_second[c] * moving[c] - from_first[c] * first[c] for c in range(3)]

    def spread(number):
        for target, terms, row, hots, tiles in (
            (own_ref, first_terms, 0, first_hot, first_tiles),
            (other_ref, second_terms, 1, second_hot, second_tiles),
        ):
            rows = []
            columns = []
            for part in range(parts):
                at = pl.multiple_of(number * block + part * LANES, LANES)
                home = jnp.broadcast_to(pair_ref[row : row + 1, pl.ds(at, LANES)] >> LANE_BITS, (16, LANES))
                home = home.astype(jnp.float32).astype(jnp.bfloat16)
                home = jnp.concatenate([home] * 3, axis=0)
                pieces = split_two(terms[part * 24 : part * 24 + 24, :])
                rows.append(jnp.concatenate([
                    jnp.where(home == jnp.bfloat16(tile), pieces, jnp.bfloat16(0)) for tile in range(tiles)
                ], axis=0))
                columns.append(hots[pl.ds(at, LANES), :])
            target[...] += lax.dot_general(
                jnp.concatenate(rows, axis=1), jnp.concatenate(columns, axis=1),
                (((1,), (1,)), ((), ())), preferred_element_type=jnp.float32,
            )

    fetch(0, 0, 0)

    def one_block(number, carry):
        spread(jnp.maximum(number - 1, 0))
        upcoming = jnp.minimum(number + 1, blocks - 1)
        virial = [virial_ref[c * 8 : c * 8 + 8, :] for c in range(3)]
        for part in range(parts):
            if part + 1 < parts:
                fetch(number, part + 1, (part + 1) % 2)
            else:
                fetch(upcoming, 0, 0)
            added = interact(number, part)
            virial = [virial[c] + added[c] for c in range(3)]
        for c in range(3):
            virial_ref[c * 8 : c * 8 + 8, :] = virial[c]
        return carry

    lax.fori_loop(0, blocks, one_block, 0)
    row = jnp.zeros((1, LANES), jnp.float32)
    for c in range(3):
        added = jnp.sum(virial_ref[c * 8 : c * 8 + 8, :], axis=0, keepdims=True)
        row = jnp.where(lane[0:1] == c, jnp.sum(added, axis=1, keepdims=True) * -0.5, row)
        row = jnp.where(lane[0:1] == c + 3, energy[c : c + 1], row)
    sum_ref[...] = row
    spread(blocks - 1)

    def sum_copy(step, source):
        return pltpu.make_async_remote_copy(
            src_ref=sum_ref, dst_ref=all_sums.at[source],
            send_sem=give_sems.at[step], recv_sem=take_sems.at[source],
            device_id={"gx": lax.rem(me + step, count)}, device_id_type=pl.DeviceIdType.MESH,
        )

    def give(step, carry):
        sum_copy(step, me).start()
        return carry

    def take(step, carry):
        sum_copy(step, lax.rem(me + count - step, count)).wait()
        return carry

    def joined(ref, tiles):
        return jnp.concatenate([
            ref[tile * 48 : tile * 48 + 24, :] + ref[tile * 48 + 24 : tile * 48 + 48, :]
            for tile in range(tiles)
        ], axis=1)

    other = joined(other_ref, second_tiles)
    own = joined(own_ref, first_tiles)
    near_push[:, 0:clusters] = other[:, clusters : 2 * clusters]
    far_push[:, 0:far_count] = other[:, 2 * clusters : slots]
    homeward = [remote(far_push, far_back, 3, 2), remote(near_push, near_back, 2, 1)]
    for copy in homeward:
        copy.start()
    lax.fori_loop(1, count, give, 0)
    all_sums[me] = sum_ref[...]
    folded_ref[:, 0:clusters] = other[:, 0:clusters] - own[:, 0:clusters]
    for copy in homeward:
        copy.wait()
    place = place_ref[...]
    for base in range(0, clusters, LANES):
        lanes = slice(base, base + LANES)
        index = place[:, lanes]
        within = (jnp.maximum(index, 0) & (LANES - 1)).astype(jnp.uint32)
        for c in range(3):
            rows8 = slice(c * 8, c * 8 + 8)
            value = folded_ref[rows8, lanes] + near_back[rows8, lanes]
            for tile in range(-(-far_count // LANES)):
                source = far_back[rows8, tile * LANES : (tile + 1) * LANES]
                picked = jnp.take_along_axis(source, within, axis=1, mode="promise_in_bounds")
                mine = (index >= tile * LANES) & (index < (tile + 1) * LANES)
                value = value + jnp.where(mine, picked, 0.0)
            folded_out[rows8, lanes] = value
    lax.fori_loop(1, count, take, 0)
    totals = lax.fori_loop(
        0, count, lambda source, held: held + all_sums[source], jnp.zeros((1, LANES), jnp.float32)
    )
    virial = [jnp.broadcast_to(totals[:, c : c + 1], (1, LANES)) for c in range(3)]
    kinetic = [jnp.broadcast_to(totals[:, c : c + 1], (1, LANES)) for c in range(3, 6)]
    energy = kinetic[0] + kinetic[1] + kinetic[2]
    volume = box_ref[0] * box_ref[1] * box_ref[2]
    ratio = 2.0 * energy / (3.0 * count * clusters * 8 * thermal_scale_unit)
    rate_out[3:4] = extended_ref[0] + reservoir_inertia_mass * (ratio - 1.0)
    for c in range(3):
        change = barostat_gain * (kinetic[c] - virial[c] - pressure_target * volume / 2.0) / (energy / 3.0)
        rate_out[c : c + 1] = extended_ref[1 + c] + change


def final_kernel(
    folded_ref, rate_ref, position_ref, velocity_ref, param_ref,
    force_out, velocity_out, position_out, coupling_out, *, clusters
):
    sublane = lax.broadcasted_iota(jnp.int32, (8, LANES), 0)
    lane = lax.broadcasted_iota(jnp.int32, (8, LANES), 1)
    wanted = sublane == (lane & 7)
    for c in range(3):
        for tile in range(clusters * 8 // LANES):
            at = tile * 16
            source = folded_ref[c * 8 : c * 8 + 8, at // LANES * LANES : at // LANES * LANES + LANES]
            index = (at % LANES + lane // 8).astype(jnp.uint32)
            picked = jnp.take_along_axis(source, index, axis=1, mode="promise_in_bounds")
            force_out[c : c + 1, tile * LANES : (tile + 1) * LANES] = jnp.sum(
                jnp.where(wanted, picked, 0.0), axis=0, keepdims=True
            )
    row = rate_ref[3:4, :]
    for c in range(3):
        row = jnp.where(lane[0:1] == c + 1, rate_ref[c : c + 1, :], row)
    coupling_out[...] = row[:, 0:4]
    rates = rate_ref[0:3, 0:1]
    damping = rate_ref[3:4, 0:1]
    velocity = velocity_ref[...]
    moved = velocity + time_step * (
        force_out[...] * param_ref[3:4, :] - (damping + rates) * velocity
    )
    velocity_out[...] = moved
    position_out[...] = position_ref[...] * (1.0 + time_step * rates) + time_step * moved


def on_device(
    positions,
    velocities,
    atom_params,
    pair_list,
    pair_count,
    exclusion,
    halo_far,
    box_lengths,
    extended_variables,
):
    clusters = positions.shape[1] // 8
    far_clusters = halo_far.shape[0]
    slots = 2 * clusters + far_clusters
    pairs = pair_list.shape[1]
    count = lax.axis_size("gx")
    block = next(b for b in (768, 512, 384, 256, 128) if pairs % b == 0)
    wide = round_up(clusters, LANES)
    wide_far = round_up(far_clusters, LANES)
    wide_slots = round_up(slots, LANES)
    vmem = pl.BlockSpec(memory_space=pltpu.VMEM)
    shape = jax.ShapeDtypeStruct(positions.shape, jnp.float32)
    f32 = lambda *dims: pltpu.VMEM(dims, jnp.float32)
    halo = halo_far[None, :]
    pinned = lambda array: pltpu.with_memory_space_constraint(array, pltpu.HBM)
    folded, rates = pl.pallas_call(
        functools.partial(step_kernel, count=count, clusters=clusters, slots=slots, block=block),
        name="step_kernel",
        out_shape=(
            jax.ShapeDtypeStruct((24, wide), jnp.float32), jax.ShapeDtypeStruct((4, LANES), jnp.float32)
        ),
        in_specs=[pl.BlockSpec(memory_space=pltpu.HBM)] * 9,
        out_specs=(vmem,) * 2,
        scratch_shapes=[
            pltpu.SMEM(box_lengths.shape, jnp.float32), pltpu.SMEM(extended_variables.shape, jnp.float32),
            pltpu.SMEM(pair_count.shape, jnp.int32),
            f32(*positions.shape), f32(*velocities.shape), f32(*atom_params.shape),
            pltpu.VMEM(pair_list.shape, jnp.int32), pltpu.VMEM(exclusion.shape, jnp.int32),
            pltpu.VMEM(halo.shape, jnp.int32),
            f32(48, wide_slots), f32(48, wide), f32(48, wide), f32(48, wide_far), f32(48, wide_far),
            f32(24, wide), f32(24, wide_far), f32(24, wide), f32(24, wide_far),
            f32(1, LANES), f32(count, 1, LANES),
            pltpu.VMEM((8, wide), jnp.int32), f32(24, wide),
            f32(pairs // LANES * 88, LANES), f32(pairs // LANES * 64, LANES), f32(pairs // LANES * 64, LANES),
pltpu.VMEM((pairs, LANES), jnp.bfloat16), pltpu.VMEM((pairs, LANES), jnp.bfloat16),
            f32(96, LANES), f32(block // LANES * 24, LANES), f32(block // LANES * 24, LANES),
            f32(wide // LANES * 48, LANES), f32(wide_slots // LANES * 48, LANES), f32(24, LANES),
            pltpu.SemaphoreType.DMA((9,)), pltpu.SemaphoreType.DMA((4,)), pltpu.SemaphoreType.DMA((4,)),
            pltpu.SemaphoreType.DMA((count,)), pltpu.SemaphoreType.DMA((count,)),
        ],
        compiler_params=pltpu.CompilerParams(
            collective_id=0, has_side_effects=True, vmem_limit_bytes=32 * 1024 * 1024
        ),
    )(
        pinned(box_lengths), pinned(extended_variables), pair_count, pinned(positions), pinned(velocities),
        pinned(atom_params), pinned(pair_list), pinned(exclusion), pinned(halo),
    )
    forces, new_velocities, new_positions, new_coupling = pl.pallas_call(
        functools.partial(final_kernel, clusters=clusters),
        name="final_kernel",
        out_shape=(shape,) * 3 + (jax.ShapeDtypeStruct((1, 4), jnp.float32),),
        in_specs=[vmem] * 5,
        out_specs=(vmem,) * 4,
        compiler_params=pltpu.CompilerParams(vmem_limit_bytes=4 * 1024 * 1024),
    )(folded, rates, positions, velocities, atom_params)
    return (forces, new_velocities, new_positions, new_coupling.reshape(4))


def solution(mesh):
    spread = P(None, ("rep", "gx"))
    return jax.shard_map(
        on_device,
        mesh=mesh,
        in_specs=(spread,) * 4 + (P(("rep", "gx")), spread, P(("rep", "gx")), P("rep"), P("rep")),
        out_specs=(spread,) * 3 + (P("rep"),),
        check_vma=False,
    )
```

```python
import functools

import jax
import jax.numpy as jnp
from jax import lax
from jax.experimental import pallas as pl
from jax.experimental.pallas import tpu as pltpu
from jax.sharding import PartitionSpec as P

time_step = 0.25
reaction_term = 1.0 / 1331.0
thermal_scale_unit = 2.0
reservoir_inertia_mass = 4.0
barostat_gain = 0.1
pressure_target = 1.0

LANES = 128
LANE_BITS = LANES.bit_length() - 1
FAR_AWAY = 1e36


def round_up(value, unit):
    return (value + unit - 1) // unit * unit


def rows_from(row):
    return slice(row, row + 8)


def split_two(value):
    high = value.astype(jnp.bfloat16).astype(jnp.float32)
    return jnp.concatenate([high, value - high], axis=0).astype(jnp.bfloat16)


def picked_rows(table_ref, index, first_tile, last_tile, held=None):
    within = (index & (LANES - 1)).astype(jnp.uint32)
    block = index >> LANE_BITS
    result = []
    for component in range(6):
        value = None if held is None else held[component]
        for tile in range(first_tile, last_tile):
            source = table_ref[component * 8 : component * 8 + 8, tile * LANES : (tile + 1) * LANES]
            picked = jnp.take_along_axis(source, within, axis=1, mode="promise_in_bounds")
            value = picked if value is None else jnp.where(block == tile, picked, value)
        result.append(value)
    return result


def step_kernel(
    box_in, extended_in, count_in, position_in, velocity_in, param_in, pair_in, word_in, halo_in,
    folded_out, rate_out, box_ref, extended_ref, count_ref,
    position_ref, velocity_ref, param_ref, pair_ref, word_ref, halo_ref,
    table_ref, packed_ref, near_got, far_send, far_got, near_push, far_push, near_back, far_back,
    sum_ref, all_sums, place_ref, folded_ref,
    first_kept, far_kept, term_kept, first_hot, second_hot,
    second_got, first_terms, second_terms, own_ref, other_ref, virial_ref,
    local_sems, send_sems, recv_sems, give_sems, take_sems,
    *, count, clusters, slots, block
):
    me = lax.axis_index("gx")
    parts = block // LANES
    pairs = pair_ref.shape[1]
    blocks = pairs // block
    far_count = slots - 2 * clusters
    first_tiles = -(-clusters // LANES)
    second_tiles = -(-slots // LANES)
    barrier = pltpu.get_barrier_semaphore()

    def greet(step, carry):
        pl.semaphore_signal(
            barrier, inc=1, device_id={"gx": lax.rem(me + step, count)},
            device_id_type=pl.DeviceIdType.MESH,
        )
        return carry

    close = sorted({1, count - 1, 2, count - 2} - {0, count})
    for step in close:
        greet(step, 0)
    lax.fori_loop(3, count - 2, greet, 0)
    inward = [
        pltpu.make_async_copy(source, target, local_sems.at[number])
        for number, (source, target) in enumerate((
            (position_in, position_ref), (param_in, param_ref), (halo_in, halo_ref),
            (pair_in, pair_ref), (word_in, word_ref), (count_in, count_ref), (box_in, box_ref),
            (velocity_in, velocity_ref), (extended_in, extended_ref),
        ))
    ]
    for copy in inward:
        copy.start()

    sublane = lax.broadcasted_iota(jnp.int32, (8, LANES), 0)
    lane = lax.broadcasted_iota(jnp.int32, (8, LANES), 1)
    own_ref[...] = jnp.zeros_like(own_ref)
    other_ref[...] = jnp.zeros_like(other_ref)
    virial_ref[...] = jnp.zeros_like(virial_ref)
    first_terms[...] = jnp.zeros_like(first_terms)
    second_terms[...] = jnp.zeros_like(second_terms)
    packed_ref[...] = jnp.zeros_like(packed_ref)
    table_ref[...] = jnp.zeros_like(table_ref)

    for copy in inward[:3]:
        copy.wait()
    place = (lane & 15) * 8 + sublane
    for component in range(6):
        source = position_ref if component < 3 else param_ref
        row = component % 3
        for start in range(0, clusters, LANES):
            width = min(LANES, clusters - start)
            value = jnp.zeros((8, LANES), jnp.float32)
            for piece in range(width // 16):
                at = start * 8 + piece * LANES
                spread = jnp.broadcast_to(source[row : row + 1, at : at + LANES], (8, LANES))
                picked = jnp.take_along_axis(spread, place, axis=1, mode="promise_in_bounds")
                value = jnp.where(lane // 16 == piece, picked, value)
            packed_ref[component * 8 : component * 8 + 8, start : start + LANES] = value
    for start in range(0, far_count, LANES):
        width = min(LANES, far_count - start)
        chosen = halo_ref[0:1, start : start + width]
        if width < LANES:
            chosen = jnp.concatenate([chosen, jnp.zeros((1, LANES - width), jnp.int32)], axis=1)
        values = picked_rows(packed_ref, jnp.broadcast_to(chosen, (8, LANES)), 0, first_tiles)
        for component in range(6):
            far_send[component * 8 : component * 8 + 8, start : start + LANES] = values[component]
    table_ref[:, 0:clusters] = packed_ref[:, 0:clusters]

    def remote(source, target, number, hops):
        return pltpu.make_async_remote_copy(
            src_ref=source, dst_ref=target,
            send_sem=send_sems.at[number], recv_sem=recv_sems.at[number],
            device_id={"gx": lax.rem(me + hops, count)}, device_id_type=pl.DeviceIdType.MESH,
        )

    pl.semaphore_wait(barrier, count - 1)
    outward = [remote(far_send, far_got, 1, count - 2), remote(packed_ref, near_got, 0, count - 1)]
    for copy in outward:
        copy.start()
    for copy in inward[3:7]:
        copy.wait()

    total = count_ref[0]
    box_y = box_ref[1]
    box_z = box_ref[2]


    ramps = [
        (lax.broadcasted_iota(jnp.int32, (16, LANES), 0) + group).astype(jnp.float32).astype(jnp.bfloat16)
        for group in range(0, LANES, 16)
    ]

    def hot(index, hots, tile):
        low = jnp.broadcast_to((index & (LANES - 1)).astype(jnp.float32), (16, LANES)).astype(jnp.bfloat16)
        for group in range(LANES // 16):
            hots[tile, group * 16 : group * 16 + 16, :] = jnp.where(
                low == ramps[group], jnp.bfloat16(1), jnp.bfloat16(0)
            )

    group_parts = next(n for n in (12, 6, 4, 3, 2, 1) if pairs // LANES % n == 0)

    def prepare(number, carry):
        for part in range(group_parts):
            tile = number * group_parts + part
            at = pl.multiple_of(tile * LANES, LANES)
            here = pl.ds(at, LANES)
            hot(pair_ref[0:1, here], first_hot, tile)
            hot(pair_ref[1:2, here], second_hot, tile)
            first = picked_rows(
                packed_ref, jnp.broadcast_to(pair_ref[0:1, here], (8, LANES)), 0, first_tiles
            )
            for c in range(3):
                origin = first[c][0:1]
                first_kept[tile, rows_from(48 + c * 8), :] = jnp.broadcast_to(origin, (8, LANES))
                first[c] = first[c] - jnp.broadcast_to(origin, (8, LANES))
            first[4] = 6.0 * first[4]
            first[5] = 12.0 * first[5]
            for c in range(6):
                first_kept[tile, rows_from(c * 8), :] = first[c]
            image = jnp.broadcast_to(pair_ref[2:3, here], (8, LANES))
            step_y = jnp.where(image >= 6, 1.0, jnp.where(image >= 3, 0.0, -1.0))
            step_z = image.astype(jnp.float32) - 3.0 * step_y - 4.0
            first_kept[tile, rows_from(72), :] = step_y * box_y
            first_kept[tile, rows_from(80), :] = step_z * box_z
            words = [jnp.broadcast_to(word_ref[w : w + 1, here], (8, LANES)) for w in range(4)]
            low = jnp.where(sublane < 2, words[0], words[1])
            high = jnp.where(sublane < 6, words[2], words[3])
            bits = jnp.where(sublane < 4, low, high) >> (8 * (sublane & 1))
            bits = jnp.where(at + lane < total, bits, 0)
            for turn in range(8):
                wanted = (bits & (1 << ((sublane + turn) & 7))) != 0
                far_kept[tile, rows_from(turn * 8), :] = jnp.where(wanted, 0.0, FAR_AWAY)
                term_kept[tile, rows_from(turn * 8), :] = jnp.where(wanted, reaction_term, 0.0)
        return carry

    lax.fori_loop(0, pairs // LANES // group_parts, prepare, 0)
    for copy in inward[7:]:
        copy.wait()
    energy = velocity_ref[...] * velocity_ref[...] / param_ref[3:4, :]
    energy = 0.5 * jnp.sum(energy, axis=1, keepdims=True)
    place_ref[...] = jnp.full_like(place_ref, -1)
    for start in range(0, far_count, LANES):
        width = min(LANES, far_count - start)
        chosen = halo_ref[0:1, start : start + width].astype(jnp.float32)
        for base in range(0, clusters, LANES):
            height = min(LANES, clusters - base)
            wanted = lax.broadcasted_iota(jnp.int32, (LANES, width), 0).astype(jnp.float32) + base
            hit = jnp.where(jnp.broadcast_to(chosen, (LANES, width)) == wanted, 1.0, 0.0)
            column = lax.broadcasted_iota(jnp.int32, (8, width), 1).astype(jnp.float32)
            found = lax.dot_general(
                jnp.concatenate([column + 1.0, jnp.zeros((8, width), jnp.float32)], axis=0).astype(jnp.bfloat16),
                hit.astype(jnp.bfloat16), (((1,), (1,)), ((), ())), preferred_element_type=jnp.float32,
            )[0:8].astype(jnp.int32)
            held = place_ref[:, base : base + LANES]
            place_ref[:, base : base + LANES] = jnp.where(found > 0, found - 1 + start, held)

    for copy in outward:
        copy.wait()
    near_lift = jnp.where(me >= count - 1, box_ref[0], 0.0)
    far_lift = jnp.where(me >= count - 2, box_ref[0], 0.0)
    upper = lax.broadcasted_iota(jnp.int32, (48, clusters), 0) < 8
    table_ref[:, clusters : 2 * clusters] = near_got[:, 0:clusters] + jnp.where(upper, near_lift, 0.0)
    upper = lax.broadcasted_iota(jnp.int32, (48, far_count), 0) < 8
    table_ref[:, 2 * clusters : slots] = far_got[:, 0:far_count] + jnp.where(upper, far_lift, 0.0)

    def fetch(number, part, slot):
        at = pl.multiple_of(number * block + part * LANES, LANES)
        here = pl.ds(at, LANES)
        tile = number * parts + part
        second = picked_rows(
            table_ref, jnp.broadcast_to(pair_ref[1:2, here], (8, LANES)), 0, second_tiles
        )
        for c in range(3):
            second[c] = second[c] - first_kept[tile, rows_from(48 + c * 8), :]
            if c:
                second[c] = second[c] + first_kept[tile, rows_from(64 + c * 8), :]
        for c in range(6):
            second_got[slot * 48 + c * 8 : slot * 48 + c * 8 + 8, :] = second[c]

    def interact(number, part):
        tile = number * parts + part
        first = [first_kept[tile, rows_from(c * 8), :] for c in range(6)]
        low = (part % 2) * 48
        charge, dispersion, repulsion = first[3], first[4], first[5]
        from_first = [None] * 3
        onto_second = [None] * 3
        for turn in range(7, -1, -1):
            moving = [second_got[low + c * 8 : low + c * 8 + 8, :] for c in range(6)]
            if turn:
                moving = [pltpu.roll(m, 8 - turn, 0) for m in moving]
            delta = [moving[c] - first[c] for c in range(3)]
            radius_sq = delta[0] * delta[0] + delta[1] * delta[1] + delta[2] * delta[2]
            inverse = lax.rsqrt(radius_sq + far_kept[tile, rows_from(turn * 8), :])
            inverse_sq = inverse * inverse
            cube = inverse * inverse_sq
            six = cube * cube
            scalar = charge * moving[3] * (cube - term_kept[tile, rows_from(turn * 8), :]) + (
                repulsion * moving[5] * six - dispersion * moving[4]
            ) * (six * inverse_sq)
            for c in range(3):
                force = scalar * delta[c]
                if from_first[c] is None:
                    from_first[c] = force
                    onto_second[c] = force
                else:
                    from_first[c] = from_first[c] + force
                    onto_second[c] = pltpu.roll(onto_second[c], 1, 0) + force
        for c in range(3):
            first_terms[part * 24 + c * 8 : part * 24 + c * 8 + 8, :] = from_first[c]
            second_terms[part * 24 + c * 8 : part * 24 + c * 8 + 8, :] = onto_second[c]
        return [onto_second[c] * moving[c] - from_first[c] * first[c] for c in range(3)]

    def spread(number):
        for target, terms, row, hots, tiles in (
            (own_ref, first_terms, 0, first_hot, first_tiles),
            (other_ref, second_terms, 1, second_hot, second_tiles),
        ):
            rows = []
            columns = []
            for part in range(parts):
                at = pl.multiple_of(number * block + part * LANES, LANES)
                home = jnp.broadcast_to(pair_ref[row : row + 1, pl.ds(at, LANES)] >> LANE_BITS, (16, LANES))
                home = home.astype(jnp.float32).astype(jnp.bfloat16)
                home = jnp.concatenate([home] * 3, axis=0)
                pieces = split_two(terms[part * 24 : part * 24 + 24, :])
                rows.append(jnp.concatenate([
                    jnp.where(home == jnp.bfloat16(tile), pieces, jnp.bfloat16(0)) for tile in range(tiles)
                ], axis=0))
                columns.append(hots[number * parts + part, :, :])
            target[...] += lax.dot_general(
                jnp.concatenate(rows, axis=1), jnp.concatenate(columns, axis=1),
                (((1,), (1,)), ((), ())), preferred_element_type=jnp.float32,
            )

    fetch(0, 0, 0)

    def one_block(number, carry):
        spread(jnp.maximum(number - 1, 0))
        upcoming = jnp.minimum(number + 1, blocks - 1)
        virial = [virial_ref[c * 8 : c * 8 + 8, :] for c in range(3)]
        for part in range(parts):
            if part + 1 < parts:
                fetch(number, part + 1, (part + 1) % 2)
            else:
                fetch(upcoming, 0, 0)
            added = interact(number, part)
            virial = [virial[c] + added[c] for c in range(3)]
        for c in range(3):
            virial_ref[c * 8 : c * 8 + 8, :] = virial[c]
        return carry

    lax.fori_loop(0, blocks, one_block, 0)
    row = jnp.zeros((1, LANES), jnp.float32)
    for c in range(3):
        added = jnp.sum(virial_ref[c * 8 : c * 8 + 8, :], axis=0, keepdims=True)
        row = jnp.where(lane[0:1] == c, jnp.sum(added, axis=1, keepdims=True) * -0.5, row)
        row = jnp.where(lane[0:1] == c + 3, energy[c : c + 1], row)
    sum_ref[...] = row
    spread(blocks - 1)

    def sum_copy(step, source):
        return pltpu.make_async_remote_copy(
            src_ref=sum_ref, dst_ref=all_sums.at[source],
            send_sem=give_sems.at[step], recv_sem=take_sems.at[source],
            device_id={"gx": lax.rem(me + step, count)}, device_id_type=pl.DeviceIdType.MESH,
        )

    def give(step, carry):
        sum_copy(step, me).start()
        return carry

    def take(step, carry):
        sum_copy(step, lax.rem(me + count - step, count)).wait()
        return carry

    def joined(ref, tiles):
        return jnp.concatenate([
            ref[tile * 48 : tile * 48 + 24, :] + ref[tile * 48 + 24 : tile * 48 + 48, :]
            for tile in range(tiles)
        ], axis=1)

    other = joined(other_ref, second_tiles)
    own = joined(own_ref, first_tiles)
    near_push[:, 0:clusters] = other[:, clusters : 2 * clusters]
    far_push[:, 0:far_count] = other[:, 2 * clusters : slots]
    homeward = [remote(far_push, far_back, 3, 2), remote(near_push, near_back, 2, 1)]
    for copy in homeward:
        copy.start()
    lax.fori_loop(1, count, give, 0)
    all_sums[me] = sum_ref[...]
    folded_ref[:, 0:clusters] = other[:, 0:clusters] - own[:, 0:clusters]
    for copy in homeward:
        copy.wait()
    place = place_ref[...]
    for base in range(0, clusters, LANES):
        lanes = slice(base, base + LANES)
        index = place[:, lanes]
        within = (jnp.maximum(index, 0) & (LANES - 1)).astype(jnp.uint32)
        for c in range(3):
            rows8 = slice(c * 8, c * 8 + 8)
            value = folded_ref[rows8, lanes] + near_back[rows8, lanes]
            for tile in range(-(-far_count // LANES)):
                source = far_back[rows8, tile * LANES : (tile + 1) * LANES]
                picked = jnp.take_along_axis(source, within, axis=1, mode="promise_in_bounds")
                mine = (index >= tile * LANES) & (index < (tile + 1) * LANES)
                value = value + jnp.where(mine, picked, 0.0)
            folded_out[rows8, lanes] = value
    lax.fori_loop(1, count, take, 0)
    totals = lax.fori_loop(
        0, count, lambda source, held: held + all_sums[source], jnp.zeros((1, LANES), jnp.float32)
    )
    virial = [jnp.broadcast_to(totals[:, c : c + 1], (1, LANES)) for c in range(3)]
    kinetic = [jnp.broadcast_to(totals[:, c : c + 1], (1, LANES)) for c in range(3, 6)]
    energy = kinetic[0] + kinetic[1] + kinetic[2]
    volume = box_ref[0] * box_ref[1] * box_ref[2]
    ratio = 2.0 * energy / (3.0 * count * clusters * 8 * thermal_scale_unit)
    rate_out[3:4] = extended_ref[0] + reservoir_inertia_mass * (ratio - 1.0)
    for c in range(3):
        change = barostat_gain * (kinetic[c] - virial[c] - pressure_target * volume / 2.0) / (energy / 3.0)
        rate_out[c : c + 1] = extended_ref[1 + c] + change


def final_kernel(
    folded_ref, rate_ref, position_ref, velocity_ref, param_ref,
    force_out, velocity_out, position_out, coupling_out, *, clusters
):
    sublane = lax.broadcasted_iota(jnp.int32, (8, LANES), 0)
    lane = lax.broadcasted_iota(jnp.int32, (8, LANES), 1)
    wanted = sublane == (lane & 7)
    for c in range(3):
        for tile in range(clusters * 8 // LANES):
            at = tile * 16
            source = folded_ref[c * 8 : c * 8 + 8, at // LANES * LANES : at // LANES * LANES + LANES]
            index = (at % LANES + lane // 8).astype(jnp.uint32)
            picked = jnp.take_along_axis(source, index, axis=1, mode="promise_in_bounds")
            force_out[c : c + 1, tile * LANES : (tile + 1) * LANES] = jnp.sum(
                jnp.where(wanted, picked, 0.0), axis=0, keepdims=True
            )
    row = rate_ref[3:4, :]
    for c in range(3):
        row = jnp.where(lane[0:1] == c + 1, rate_ref[c : c + 1, :], row)
    coupling_out[...] = row[:, 0:4]
    rates = rate_ref[0:3, 0:1]
    damping = rate_ref[3:4, 0:1]
    velocity = velocity_ref[...]
    moved = velocity + time_step * (
        force_out[...] * param_ref[3:4, :] - (damping + rates) * velocity
    )
    velocity_out[...] = moved
    position_out[...] = position_ref[...] * (1.0 + time_step * rates) + time_step * moved


def on_device(
    positions,
    velocities,
    atom_params,
    pair_list,
    pair_count,
    exclusion,
    halo_far,
    box_lengths,
    extended_variables,
):
    clusters = positions.shape[1] // 8
    far_clusters = halo_far.shape[0]
    slots = 2 * clusters + far_clusters
    pairs = pair_list.shape[1]
    count = lax.axis_size("gx")
    block = next(b for b in (768, 512, 384, 256, 128) if pairs % b == 0)
    wide = round_up(clusters, LANES)
    wide_far = round_up(far_clusters, LANES)
    wide_slots = round_up(slots, LANES)
    vmem = pl.BlockSpec(memory_space=pltpu.VMEM)
    shape = jax.ShapeDtypeStruct(positions.shape, jnp.float32)
    f32 = lambda *dims: pltpu.VMEM(dims, jnp.float32)
    halo = halo_far[None, :]
    pinned = lambda array: pltpu.with_memory_space_constraint(array, pltpu.HBM)
    folded, rates = pl.pallas_call(
        functools.partial(step_kernel, count=count, clusters=clusters, slots=slots, block=block),
        name="step_kernel",
        out_shape=(
            jax.ShapeDtypeStruct((24, wide), jnp.float32), jax.ShapeDtypeStruct((4, LANES), jnp.float32)
        ),
        in_specs=[pl.BlockSpec(memory_space=pltpu.HBM)] * 9,
        out_specs=(vmem,) * 2,
        scratch_shapes=[
            pltpu.SMEM(box_lengths.shape, jnp.float32), pltpu.SMEM(extended_variables.shape, jnp.float32),
            pltpu.SMEM(pair_count.shape, jnp.int32),
            f32(*positions.shape), f32(*velocities.shape), f32(*atom_params.shape),
            pltpu.VMEM(pair_list.shape, jnp.int32), pltpu.VMEM(exclusion.shape, jnp.int32),
            pltpu.VMEM(halo.shape, jnp.int32),
            f32(48, wide_slots), f32(48, wide), f32(48, wide), f32(48, wide_far), f32(48, wide_far),
            f32(24, wide), f32(24, wide_far), f32(24, wide), f32(24, wide_far),
            f32(1, LANES), f32(count, 1, LANES),
            pltpu.VMEM((8, wide), jnp.int32), f32(24, wide),
            f32(pairs // LANES, 88, LANES), f32(pairs // LANES, 64, LANES), f32(pairs // LANES, 64, LANES),
pltpu.VMEM((pairs // LANES, LANES, LANES), jnp.bfloat16),
            pltpu.VMEM((pairs // LANES, LANES, LANES), jnp.bfloat16),
            f32(96, LANES), f32(block // LANES * 24, LANES), f32(block // LANES * 24, LANES),
            f32(wide // LANES * 48, LANES), f32(wide_slots // LANES * 48, LANES), f32(24, LANES),
            pltpu.SemaphoreType.DMA((9,)), pltpu.SemaphoreType.DMA((4,)), pltpu.SemaphoreType.DMA((4,)),
            pltpu.SemaphoreType.DMA((count,)), pltpu.SemaphoreType.DMA((count,)),
        ],
        compiler_params=pltpu.CompilerParams(
            collective_id=0, has_side_effects=True, vmem_limit_bytes=32 * 1024 * 1024
        ),
    )(
        pinned(box_lengths), pinned(extended_variables), pair_count, pinned(positions), pinned(velocities),
        pinned(atom_params), pinned(pair_list), pinned(exclusion), pinned(halo),
    )
    forces, new_velocities, new_positions, new_coupling = pl.pallas_call(
        functools.partial(final_kernel, clusters=clusters),
        name="final_kernel",
        out_shape=(shape,) * 3 + (jax.ShapeDtypeStruct((1, 4), jnp.float32),),
        in_specs=[vmem] * 5,
        out_specs=(vmem,) * 4,
        compiler_params=pltpu.CompilerParams(vmem_limit_bytes=4 * 1024 * 1024),
    )(folded, rates, positions, velocities, atom_params)
    return (forces, new_velocities, new_positions, new_coupling.reshape(4))


def solution(mesh):
    spread = P(None, ("rep", "gx"))
    return jax.shard_map(
        on_device,
        mesh=mesh,
        in_specs=(spread,) * 4 + (P(("rep", "gx")), spread, P(("rep", "gx")), P("rep"), P("rep")),
        out_specs=(spread,) * 3 + (P("rep"),),
        check_vma=False,
    )
```

```python
import functools

import jax
import jax.numpy as jnp
from jax import lax
from jax.experimental import pallas as pl
from jax.experimental.pallas import tpu as pltpu
from jax.sharding import PartitionSpec as P

time_step = 0.25
reaction_term = 1.0 / 1331.0
thermal_scale_unit = 2.0
reservoir_inertia_mass = 4.0
barostat_gain = 0.1
pressure_target = 1.0

LANES = 128
LANE_BITS = LANES.bit_length() - 1
FAR_AWAY = 1e36


def round_up(value, unit):
    return (value + unit - 1) // unit * unit


def rows_from(row):
    return slice(row, row + 8)


def split_two(value):
    high = value.astype(jnp.bfloat16).astype(jnp.float32)
    return jnp.concatenate([high, value - high], axis=0).astype(jnp.bfloat16)


def picked_rows(table_ref, index, first_tile, last_tile, held=None):
    within = (index & (LANES - 1)).astype(jnp.uint32)
    block = index >> LANE_BITS
    result = []
    for component in range(6):
        value = None if held is None else held[component]
        for tile in range(first_tile, last_tile):
            source = table_ref[component * 8 : component * 8 + 8, tile * LANES : (tile + 1) * LANES]
            picked = jnp.take_along_axis(source, within, axis=1, mode="promise_in_bounds")
            value = picked if value is None else jnp.where(block == tile, picked, value)
        result.append(value)
    return result


def step_kernel(
    box_in, extended_in, count_in, position_in, velocity_in, param_in, pair_in, word_in, halo_in,
    folded_out, rate_out, box_ref, extended_ref, count_ref,
    position_ref, velocity_ref, param_ref, pair_ref, word_ref, halo_ref,
    table_ref, packed_ref, near_got, far_send, far_got, near_push, far_push, near_back, far_back,
    sum_ref, all_sums, place_ref, folded_ref,
    first_kept, far_kept, term_kept, first_hot, second_hot,
    second_got, first_terms, second_terms, own_ref, other_ref, virial_ref,
    local_sems, send_sems, recv_sems, give_sems, take_sems,
    *, count, clusters, slots, block
):
    me = lax.axis_index("gx")
    parts = block // LANES
    pairs = pair_ref.shape[1]
    blocks = pairs // block
    far_count = slots - 2 * clusters
    first_tiles = -(-clusters // LANES)
    second_tiles = -(-slots // LANES)
    barrier = pltpu.get_barrier_semaphore()

    def greet(step, carry):
        pl.semaphore_signal(
            barrier, inc=1, device_id={"gx": lax.rem(me + step, count)},
            device_id_type=pl.DeviceIdType.MESH,
        )
        return carry

    close = sorted({1, count - 1, 2, count - 2} - {0, count})
    for step in close:
        greet(step, 0)
    lax.fori_loop(3, count - 2, greet, 0)
    inward = [
        pltpu.make_async_copy(source, target, local_sems.at[number])
        for number, (source, target) in enumerate((
            (position_in, position_ref), (param_in, param_ref), (halo_in, halo_ref),
            (pair_in, pair_ref), (word_in, word_ref), (count_in, count_ref), (box_in, box_ref),
            (velocity_in, velocity_ref), (extended_in, extended_ref),
        ))
    ]
    for copy in inward:
        copy.start()

    sublane = lax.broadcasted_iota(jnp.int32, (8, LANES), 0)
    lane = lax.broadcasted_iota(jnp.int32, (8, LANES), 1)
    own_ref[...] = jnp.zeros_like(own_ref)
    other_ref[...] = jnp.zeros_like(other_ref)
    virial_ref[...] = jnp.zeros_like(virial_ref)
    first_terms[...] = jnp.zeros_like(first_terms)
    second_terms[...] = jnp.zeros_like(second_terms)
    packed_ref[...] = jnp.zeros_like(packed_ref)
    table_ref[...] = jnp.zeros_like(table_ref)

    for copy in inward[:3]:
        copy.wait()
    place = (lane & 15) * 8 + sublane
    for component in range(6):
        source = position_ref if component < 3 else param_ref
        row = component % 3
        for start in range(0, clusters, LANES):
            width = min(LANES, clusters - start)
            value = jnp.zeros((8, LANES), jnp.float32)
            for piece in range(width // 16):
                at = start * 8 + piece * LANES
                spread = jnp.broadcast_to(source[row : row + 1, at : at + LANES], (8, LANES))
                picked = jnp.take_along_axis(spread, place, axis=1, mode="promise_in_bounds")
                value = jnp.where(lane // 16 == piece, picked, value)
            packed_ref[component * 8 : component * 8 + 8, start : start + LANES] = value
    for start in range(0, far_count, LANES):
        width = min(LANES, far_count - start)
        chosen = halo_ref[0:1, start : start + width]
        if width < LANES:
            chosen = jnp.concatenate([chosen, jnp.zeros((1, LANES - width), jnp.int32)], axis=1)
        values = picked_rows(packed_ref, jnp.broadcast_to(chosen, (8, LANES)), 0, first_tiles)
        for component in range(6):
            far_send[component * 8 : component * 8 + 8, start : start + LANES] = values[component]
    table_ref[:, 0:clusters] = packed_ref[:, 0:clusters]

    def remote(source, target, number, hops):
        return pltpu.make_async_remote_copy(
            src_ref=source, dst_ref=target,
            send_sem=send_sems.at[number], recv_sem=recv_sems.at[number],
            device_id={"gx": lax.rem(me + hops, count)}, device_id_type=pl.DeviceIdType.MESH,
        )

    pl.semaphore_wait(barrier, count - 1)
    outward = [remote(far_send, far_got, 1, count - 2), remote(packed_ref, near_got, 0, count - 1)]
    for copy in outward:
        copy.start()
    for copy in inward[3:7]:
        copy.wait()

    total = count_ref[0]
    box_y = box_ref[1]
    box_z = box_ref[2]


    ramps = [
        (lax.broadcasted_iota(jnp.int32, (16, LANES), 0) + group).astype(jnp.float32).astype(jnp.bfloat16)
        for group in range(0, LANES, 16)
    ]

    def hot(index, hots, tile):
        low = jnp.broadcast_to((index & (LANES - 1)).astype(jnp.float32), (16, LANES)).astype(jnp.bfloat16)
        for group in range(LANES // 16):
            hots[tile, group * 16 : group * 16 + 16, :] = jnp.where(
                low == ramps[group], jnp.bfloat16(1), jnp.bfloat16(0)
            )

    group_parts = next(n for n in (12, 6, 4, 3, 2, 1) if pairs // LANES % n == 0)

    def prepare(number, carry):
        for part in range(group_parts):
            tile = number * group_parts + part
            at = pl.multiple_of(tile * LANES, LANES)
            here = pl.ds(at, LANES)
            hot(pair_ref[0:1, here], first_hot, tile)
            hot(pair_ref[1:2, here], second_hot, tile)
            first = picked_rows(
                packed_ref, jnp.broadcast_to(pair_ref[0:1, here], (8, LANES)), 0, first_tiles
            )
            for c in range(3):
                origin = jnp.broadcast_to(first[c][0:1], (8, LANES))
                first_kept[tile, rows_from(384 + c * 8), :] = origin
                first[c] = first[c] - origin
            first[4] = 6.0 * first[4]
            first[5] = 12.0 * first[5]
            for turn in range(8):
                for c in range(6):
                    turned = pltpu.roll(first[c], 8 - turn, 0) if turn else first[c]
                    first_kept[tile, rows_from(turn * 48 + c * 8), :] = turned
            image = jnp.broadcast_to(pair_ref[2:3, here], (8, LANES))
            step_y = jnp.where(image >= 6, 1.0, jnp.where(image >= 3, 0.0, -1.0))
            step_z = image.astype(jnp.float32) - 3.0 * step_y - 4.0
            first_kept[tile, rows_from(408), :] = step_y * box_y
            first_kept[tile, rows_from(416), :] = step_z * box_z
            words = [jnp.broadcast_to(word_ref[w : w + 1, here], (8, LANES)) for w in range(4)]
            low = jnp.where(sublane < 2, words[0], words[1])
            high = jnp.where(sublane < 6, words[2], words[3])
            bits = jnp.where(sublane < 4, low, high) >> (8 * (sublane & 1))
            bits = jnp.where(at + lane < total, bits, 0)
            for turn in range(8):
                turned = pltpu.roll(bits, 8 - turn, 0) if turn else bits
                wanted = (turned & (1 << sublane)) != 0
                far_kept[tile, rows_from(turn * 8), :] = jnp.where(wanted, 0.0, FAR_AWAY)
                term_kept[tile, rows_from(turn * 8), :] = jnp.where(wanted, reaction_term, 0.0)
        return carry

    lax.fori_loop(0, pairs // LANES // group_parts, prepare, 0)
    for copy in inward[7:]:
        copy.wait()
    energy = velocity_ref[...] * velocity_ref[...] / param_ref[3:4, :]
    energy = 0.5 * jnp.sum(energy, axis=1, keepdims=True)
    place_ref[...] = jnp.full_like(place_ref, -1)
    for start in range(0, far_count, LANES):
        width = min(LANES, far_count - start)
        chosen = halo_ref[0:1, start : start + width].astype(jnp.float32)
        for base in range(0, clusters, LANES):
            height = min(LANES, clusters - base)
            wanted = lax.broadcasted_iota(jnp.int32, (LANES, width), 0).astype(jnp.float32) + base
            hit = jnp.where(jnp.broadcast_to(chosen, (LANES, width)) == wanted, 1.0, 0.0)
            column = lax.broadcasted_iota(jnp.int32, (8, width), 1).astype(jnp.float32)
            found = lax.dot_general(
                jnp.concatenate([column + 1.0, jnp.zeros((8, width), jnp.float32)], axis=0).astype(jnp.bfloat16),
                hit.astype(jnp.bfloat16), (((1,), (1,)), ((), ())), preferred_element_type=jnp.float32,
            )[0:8].astype(jnp.int32)
            held = place_ref[:, base : base + LANES]
            place_ref[:, base : base + LANES] = jnp.where(found > 0, found - 1 + start, held)

    for copy in outward:
        copy.wait()
    near_lift = jnp.where(me >= count - 1, box_ref[0], 0.0)
    far_lift = jnp.where(me >= count - 2, box_ref[0], 0.0)
    upper = lax.broadcasted_iota(jnp.int32, (48, clusters), 0) < 8
    table_ref[:, clusters : 2 * clusters] = near_got[:, 0:clusters] + jnp.where(upper, near_lift, 0.0)
    upper = lax.broadcasted_iota(jnp.int32, (48, far_count), 0) < 8
    table_ref[:, 2 * clusters : slots] = far_got[:, 0:far_count] + jnp.where(upper, far_lift, 0.0)

    def fetch(number, part, slot):
        at = pl.multiple_of(number * block + part * LANES, LANES)
        here = pl.ds(at, LANES)
        tile = number * parts + part
        second = picked_rows(
            table_ref, jnp.broadcast_to(pair_ref[1:2, here], (8, LANES)), 0, second_tiles
        )
        for c in range(3):
            second[c] = second[c] - first_kept[tile, rows_from(384 + c * 8), :]
            if c:
                second[c] = second[c] + first_kept[tile, rows_from(400 + c * 8), :]
        for c in range(6):
            second_got[slot * 48 + c * 8 : slot * 48 + c * 8 + 8, :] = second[c]

    def interact(number, part):
        tile = number * parts + part
        low = (part % 2) * 48
        second = [second_got[low + c * 8 : low + c * 8 + 8, :] for c in range(6)]
        from_first = [None] * 3
        onto_second = [None] * 3
        for turn in range(7, -1, -1):
            first = [first_kept[tile, rows_from(turn * 48 + c * 8), :] for c in range(6)]
            delta = [second[c] - first[c] for c in range(3)]
            radius_sq = delta[0] * delta[0] + delta[1] * delta[1] + delta[2] * delta[2]
            inverse = lax.rsqrt(radius_sq + far_kept[tile, rows_from(turn * 8), :])
            inverse_sq = inverse * inverse
            cube = inverse * inverse_sq
            six = cube * cube
            scalar = first[3] * second[3] * (cube - term_kept[tile, rows_from(turn * 8), :]) + (
                first[5] * second[5] * six - first[4] * second[4]
            ) * (six * inverse_sq)
            for c in range(3):
                force = scalar * delta[c]
                if onto_second[c] is None:
                    from_first[c] = force
                    onto_second[c] = force
                else:
                    from_first[c] = pltpu.roll(from_first[c], 1, 0) + force
                    onto_second[c] = onto_second[c] + force
        for c in range(3):
            first_terms[part * 24 + c * 8 : part * 24 + c * 8 + 8, :] = from_first[c]
            second_terms[part * 24 + c * 8 : part * 24 + c * 8 + 8, :] = onto_second[c]
        return [onto_second[c] * second[c] - from_first[c] * first[c] for c in range(3)]

    def spread(number):
        for target, terms, row, hots, tiles in (
            (own_ref, first_terms, 0, first_hot, first_tiles),
            (other_ref, second_terms, 1, second_hot, second_tiles),
        ):
            rows = []
            columns = []
            for part in range(parts):
                at = pl.multiple_of(number * block + part * LANES, LANES)
                home = jnp.broadcast_to(pair_ref[row : row + 1, pl.ds(at, LANES)] >> LANE_BITS, (16, LANES))
                home = home.astype(jnp.float32).astype(jnp.bfloat16)
                home = jnp.concatenate([home] * 3, axis=0)
                pieces = split_two(terms[part * 24 : part * 24 + 24, :])
                rows.append(jnp.concatenate([
                    jnp.where(home == jnp.bfloat16(tile), pieces, jnp.bfloat16(0)) for tile in range(tiles)
                ], axis=0))
                columns.append(hots[number * parts + part, :, :])
            target[...] += lax.dot_general(
                jnp.concatenate(rows, axis=1), jnp.concatenate(columns, axis=1),
                (((1,), (1,)), ((), ())), preferred_element_type=jnp.float32,
            )

    fetch(0, 0, 0)

    def one_block(number, carry):
        spread(jnp.maximum(number - 1, 0))
        upcoming = jnp.minimum(number + 1, blocks - 1)
        virial = [virial_ref[c * 8 : c * 8 + 8, :] for c in range(3)]
        for part in range(parts):
            if part + 1 < parts:
                fetch(number, part + 1, (part + 1) % 2)
            else:
                fetch(upcoming, 0, 0)
            added = interact(number, part)
            virial = [virial[c] + added[c] for c in range(3)]
        for c in range(3):
            virial_ref[c * 8 : c * 8 + 8, :] = virial[c]
        return carry

    lax.fori_loop(0, blocks, one_block, 0)
    row = jnp.zeros((1, LANES), jnp.float32)
    for c in range(3):
        added = jnp.sum(virial_ref[c * 8 : c * 8 + 8, :], axis=0, keepdims=True)
        row = jnp.where(lane[0:1] == c, jnp.sum(added, axis=1, keepdims=True) * -0.5, row)
        row = jnp.where(lane[0:1] == c + 3, energy[c : c + 1], row)
    sum_ref[...] = row
    spread(blocks - 1)

    def sum_copy(step, source):
        return pltpu.make_async_remote_copy(
            src_ref=sum_ref, dst_ref=all_sums.at[source],
            send_sem=give_sems.at[step], recv_sem=take_sems.at[source],
            device_id={"gx": lax.rem(me + step, count)}, device_id_type=pl.DeviceIdType.MESH,
        )

    def give(step, carry):
        sum_copy(step, me).start()
        return carry

    def take(step, carry):
        sum_copy(step, lax.rem(me + count - step, count)).wait()
        return carry

    def joined(ref, tiles):
        return jnp.concatenate([
            ref[tile * 48 : tile * 48 + 24, :] + ref[tile * 48 + 24 : tile * 48 + 48, :]
            for tile in range(tiles)
        ], axis=1)

    other = joined(other_ref, second_tiles)
    own = joined(own_ref, first_tiles)
    near_push[:, 0:clusters] = other[:, clusters : 2 * clusters]
    far_push[:, 0:far_count] = other[:, 2 * clusters : slots]
    homeward = [remote(far_push, far_back, 3, 2), remote(near_push, near_back, 2, 1)]
    for copy in homeward:
        copy.start()
    lax.fori_loop(1, count, give, 0)
    all_sums[me] = sum_ref[...]
    folded_ref[:, 0:clusters] = other[:, 0:clusters] - own[:, 0:clusters]
    for copy in homeward:
        copy.wait()
    place = place_ref[...]
    for base in range(0, clusters, LANES):
        lanes = slice(base, base + LANES)
        index = place[:, lanes]
        within = (jnp.maximum(index, 0) & (LANES - 1)).astype(jnp.uint32)
        for c in range(3):
            rows8 = slice(c * 8, c * 8 + 8)
            value = folded_ref[rows8, lanes] + near_back[rows8, lanes]
            for tile in range(-(-far_count // LANES)):
                source = far_back[rows8, tile * LANES : (tile + 1) * LANES]
                picked = jnp.take_along_axis(source, within, axis=1, mode="promise_in_bounds")
                mine = (index >= tile * LANES) & (index < (tile + 1) * LANES)
                value = value + jnp.where(mine, picked, 0.0)
            folded_out[rows8, lanes] = value
    lax.fori_loop(1, count, take, 0)
    totals = lax.fori_loop(
        0, count, lambda source, held: held + all_sums[source], jnp.zeros((1, LANES), jnp.float32)
    )
    virial = [jnp.broadcast_to(totals[:, c : c + 1], (1, LANES)) for c in range(3)]
    kinetic = [jnp.broadcast_to(totals[:, c : c + 1], (1, LANES)) for c in range(3, 6)]
    energy = kinetic[0] + kinetic[1] + kinetic[2]
    volume = box_ref[0] * box_ref[1] * box_ref[2]
    ratio = 2.0 * energy / (3.0 * count * clusters * 8 * thermal_scale_unit)
    rate_out[3:4] = extended_ref[0] + reservoir_inertia_mass * (ratio - 1.0)
    for c in range(3):
        change = barostat_gain * (kinetic[c] - virial[c] - pressure_target * volume / 2.0) / (energy / 3.0)
        rate_out[c : c + 1] = extended_ref[1 + c] + change


def final_kernel(
    folded_ref, rate_ref, position_ref, velocity_ref, param_ref,
    force_out, velocity_out, position_out, coupling_out, *, clusters
):
    sublane = lax.broadcasted_iota(jnp.int32, (8, LANES), 0)
    lane = lax.broadcasted_iota(jnp.int32, (8, LANES), 1)
    wanted = sublane == (lane & 7)
    for c in range(3):
        for tile in range(clusters * 8 // LANES):
            at = tile * 16
            source = folded_ref[c * 8 : c * 8 + 8, at // LANES * LANES : at // LANES * LANES + LANES]
            index = (at % LANES + lane // 8).astype(jnp.uint32)
            picked = jnp.take_along_axis(source, index, axis=1, mode="promise_in_bounds")
            force_out[c : c + 1, tile * LANES : (tile + 1) * LANES] = jnp.sum(
                jnp.where(wanted, picked, 0.0), axis=0, keepdims=True
            )
    row = rate_ref[3:4, :]
    for c in range(3):
        row = jnp.where(lane[0:1] == c + 1, rate_ref[c : c + 1, :], row)
    coupling_out[...] = row[:, 0:4]
    rates = rate_ref[0:3, 0:1]
    damping = rate_ref[3:4, 0:1]
    velocity = velocity_ref[...]
    moved = velocity + time_step * (
        force_out[...] * param_ref[3:4, :] - (damping + rates) * velocity
    )
    velocity_out[...] = moved
    position_out[...] = position_ref[...] * (1.0 + time_step * rates) + time_step * moved


def on_device(
    positions,
    velocities,
    atom_params,
    pair_list,
    pair_count,
    exclusion,
    halo_far,
    box_lengths,
    extended_variables,
):
    clusters = positions.shape[1] // 8
    far_clusters = halo_far.shape[0]
    slots = 2 * clusters + far_clusters
    pairs = pair_list.shape[1]
    count = lax.axis_size("gx")
    block = next(b for b in (768, 512, 256) if pairs % b == 0)
    wide = round_up(clusters, LANES)
    wide_far = round_up(far_clusters, LANES)
    wide_slots = round_up(slots, LANES)
    vmem = pl.BlockSpec(memory_space=pltpu.VMEM)
    shape = jax.ShapeDtypeStruct(positions.shape, jnp.float32)
    f32 = lambda *dims: pltpu.VMEM(dims, jnp.float32)
    halo = halo_far[None, :]
    pinned = lambda array: pltpu.with_memory_space_constraint(array, pltpu.HBM)
    folded, rates = pl.pallas_call(
        functools.partial(step_kernel, count=count, clusters=clusters, slots=slots, block=block),
        name="step_kernel",
        out_shape=(
            jax.ShapeDtypeStruct((24, wide), jnp.float32), jax.ShapeDtypeStruct((4, LANES), jnp.float32)
        ),
        in_specs=[pl.BlockSpec(memory_space=pltpu.HBM)] * 9,
        out_specs=(vmem,) * 2,
        scratch_shapes=[
            pltpu.SMEM(box_lengths.shape, jnp.float32), pltpu.SMEM(extended_variables.shape, jnp.float32),
            pltpu.SMEM(pair_count.shape, jnp.int32),
            f32(*positions.shape), f32(*velocities.shape), f32(*atom_params.shape),
            pltpu.VMEM(pair_list.shape, jnp.int32), pltpu.VMEM(exclusion.shape, jnp.int32),
            pltpu.VMEM(halo.shape, jnp.int32),
            f32(48, wide_slots), f32(48, wide), f32(48, wide), f32(48, wide_far), f32(48, wide_far),
            f32(24, wide), f32(24, wide_far), f32(24, wide), f32(24, wide_far),
            f32(1, LANES), f32(count, 1, LANES),
            pltpu.VMEM((8, wide), jnp.int32), f32(24, wide),
            f32(pairs // LANES, 424, LANES), f32(pairs // LANES, 64, LANES), f32(pairs // LANES, 64, LANES),
pltpu.VMEM((pairs // LANES, LANES, LANES), jnp.bfloat16),
            pltpu.VMEM((pairs // LANES, LANES, LANES), jnp.bfloat16),
            f32(96, LANES), f32(block // LANES * 24, LANES), f32(block // LANES * 24, LANES),
            f32(wide // LANES * 48, LANES), f32(wide_slots // LANES * 48, LANES), f32(24, LANES),
            pltpu.SemaphoreType.DMA((9,)), pltpu.SemaphoreType.DMA((4,)), pltpu.SemaphoreType.DMA((4,)),
            pltpu.SemaphoreType.DMA((count,)), pltpu.SemaphoreType.DMA((count,)),
        ],
        compiler_params=pltpu.CompilerParams(
            collective_id=0, has_side_effects=True, vmem_limit_bytes=48 * 1024 * 1024
        ),
    )(
        pinned(box_lengths), pinned(extended_variables), pair_count, pinned(positions), pinned(velocities),
        pinned(atom_params), pinned(pair_list), pinned(exclusion), pinned(halo),
    )
    forces, new_velocities, new_positions, new_coupling = pl.pallas_call(
        functools.partial(final_kernel, clusters=clusters),
        name="final_kernel",
        out_shape=(shape,) * 3 + (jax.ShapeDtypeStruct((1, 4), jnp.float32),),
        in_specs=[vmem] * 5,
        out_specs=(vmem,) * 4,
        compiler_params=pltpu.CompilerParams(vmem_limit_bytes=4 * 1024 * 1024),
    )(folded, rates, positions, velocities, atom_params)
    return (forces, new_velocities, new_positions, new_coupling.reshape(4))


def solution(mesh):
    spread = P(None, ("rep", "gx"))
    return jax.shard_map(
        on_device,
        mesh=mesh,
        in_specs=(spread,) * 4 + (P(("rep", "gx")), spread, P(("rep", "gx")), P("rep"), P("rep")),
        out_specs=(spread,) * 3 + (P("rep"),),
        check_vma=False,
    )
```

```python
import functools

import jax
import jax.numpy as jnp
from jax import lax
from jax.experimental import pallas as pl
from jax.experimental.pallas import tpu as pltpu
from jax.sharding import PartitionSpec as P

time_step = 0.25
reaction_term = 1.0 / 1331.0
thermal_scale_unit = 2.0
reservoir_inertia_mass = 4.0
barostat_gain = 0.1
pressure_target = 1.0

LANES = 128
LANE_BITS = LANES.bit_length() - 1
FAR_AWAY = 1e36


def round_up(value, unit):
    return (value + unit - 1) // unit * unit


def rows_from(row):
    return slice(row, row + 8)


def split_two(value):
    high = value.astype(jnp.bfloat16).astype(jnp.float32)
    return jnp.concatenate([high, value - high], axis=0).astype(jnp.bfloat16)


def picked_rows(table_ref, index, first_tile, last_tile, held=None):
    within = (index & (LANES - 1)).astype(jnp.uint32)
    block = index >> LANE_BITS
    result = []
    for component in range(6):
        value = None if held is None else held[component]
        for tile in range(first_tile, last_tile):
            source = table_ref[component * 8 : component * 8 + 8, tile * LANES : (tile + 1) * LANES]
            picked = jnp.take_along_axis(source, within, axis=1, mode="promise_in_bounds")
            value = picked if value is None else jnp.where(block == tile, picked, value)
        result.append(value)
    return result


def step_kernel(
    box_in, extended_in, count_in, position_in, velocity_in, param_in, pair_in, word_in, halo_in,
    folded_out, rate_out, box_ref, extended_ref, count_ref,
    position_ref, velocity_ref, param_ref, pair_ref, word_ref, halo_ref,
    table_ref, packed_ref, near_got, far_send, far_got, near_push, far_push, near_back, far_back,
    sum_ref, all_sums, place_ref, folded_ref,
    first_kept, far_kept, term_kept, first_hot, second_hot,
    second_got, first_terms, second_terms, own_ref, other_ref, virial_ref,
    local_sems, send_sems, recv_sems, give_sems, take_sems,
    *, count, clusters, slots, block
):
    me = lax.axis_index("gx")
    parts = block // LANES
    pairs = pair_ref.shape[1]
    blocks = pairs // block
    far_count = slots - 2 * clusters
    first_tiles = -(-clusters // LANES)
    second_tiles = -(-slots // LANES)
    barrier = pltpu.get_barrier_semaphore()

    def greet(step, carry):
        pl.semaphore_signal(
            barrier, inc=1, device_id={"gx": lax.rem(me + step, count)},
            device_id_type=pl.DeviceIdType.MESH,
        )
        return carry

    close = sorted({1, count - 1, 2, count - 2} - {0, count})
    for step in close:
        greet(step, 0)
    lax.fori_loop(3, count - 2, greet, 0)
    inward = [
        pltpu.make_async_copy(source, target, local_sems.at[number])
        for number, (source, target) in enumerate((
            (position_in, position_ref), (param_in, param_ref), (halo_in, halo_ref),
            (pair_in, pair_ref), (word_in, word_ref), (count_in, count_ref), (box_in, box_ref),
            (velocity_in, velocity_ref), (extended_in, extended_ref),
        ))
    ]
    for copy in inward:
        copy.start()

    sublane = lax.broadcasted_iota(jnp.int32, (8, LANES), 0)
    lane = lax.broadcasted_iota(jnp.int32, (8, LANES), 1)
    own_ref[...] = jnp.zeros_like(own_ref)
    other_ref[...] = jnp.zeros_like(other_ref)
    virial_ref[...] = jnp.zeros_like(virial_ref)
    first_terms[...] = jnp.zeros_like(first_terms)
    second_terms[...] = jnp.zeros_like(second_terms)
    packed_ref[...] = jnp.zeros_like(packed_ref)
    table_ref[...] = jnp.zeros_like(table_ref)

    for copy in inward[:3]:
        copy.wait()
    place = (lane & 15) * 8 + sublane
    for component in range(6):
        source = position_ref if component < 3 else param_ref
        row = component % 3
        for start in range(0, clusters, LANES):
            width = min(LANES, clusters - start)
            value = jnp.zeros((8, LANES), jnp.float32)
            for piece in range(width // 16):
                at = start * 8 + piece * LANES
                spread = jnp.broadcast_to(source[row : row + 1, at : at + LANES], (8, LANES))
                picked = jnp.take_along_axis(spread, place, axis=1, mode="promise_in_bounds")
                value = jnp.where(lane // 16 == piece, picked, value)
            packed_ref[component * 8 : component * 8 + 8, start : start + LANES] = value
    for start in range(0, far_count, LANES):
        width = min(LANES, far_count - start)
        chosen = halo_ref[0:1, start : start + width]
        if width < LANES:
            chosen = jnp.concatenate([chosen, jnp.zeros((1, LANES - width), jnp.int32)], axis=1)
        values = picked_rows(packed_ref, jnp.broadcast_to(chosen, (8, LANES)), 0, first_tiles)
        for component in range(6):
            far_send[component * 8 : component * 8 + 8, start : start + LANES] = values[component]
    table_ref[:, 0:clusters] = packed_ref[:, 0:clusters]

    def remote(source, target, number, hops):
        return pltpu.make_async_remote_copy(
            src_ref=source, dst_ref=target,
            send_sem=send_sems.at[number], recv_sem=recv_sems.at[number],
            device_id={"gx": lax.rem(me + hops, count)}, device_id_type=pl.DeviceIdType.MESH,
        )

    pl.semaphore_wait(barrier, count - 1)
    outward = [remote(far_send, far_got, 1, count - 2), remote(packed_ref, near_got, 0, count - 1)]
    for copy in outward:
        copy.start()
    for copy in inward[3:7]:
        copy.wait()

    total = count_ref[0]
    box_y = box_ref[1]
    box_z = box_ref[2]


    ramps = [
        (lax.broadcasted_iota(jnp.int32, (16, LANES), 0) + group).astype(jnp.float32).astype(jnp.bfloat16)
        for group in range(0, LANES, 16)
    ]

    def hot(index, hots, tile):
        low = jnp.broadcast_to((index & (LANES - 1)).astype(jnp.float32), (16, LANES)).astype(jnp.bfloat16)
        for group in range(LANES // 16):
            hots[tile, group * 16 : group * 16 + 16, :] = jnp.where(
                low == ramps[group], jnp.bfloat16(1), jnp.bfloat16(0)
            )

    group_parts = next(n for n in (12, 6, 4, 3, 2, 1) if pairs // LANES % n == 0)

    def prepare(number, carry):
        for part in range(group_parts):
            tile = number * group_parts + part
            at = pl.multiple_of(tile * LANES, LANES)
            here = pl.ds(at, LANES)
            hot(pair_ref[0:1, here], first_hot, tile)
            hot(pair_ref[1:2, here], second_hot, tile)
            first = picked_rows(
                packed_ref, jnp.broadcast_to(pair_ref[0:1, here], (8, LANES)), 0, first_tiles
            )
            for c in range(3):
                origin = jnp.broadcast_to(first[c][0:1], (8, LANES))
                first_kept[tile, rows_from(384 + c * 8), :] = origin
                first[c] = first[c] - origin
            first[4] = 6.0 * first[4]
            first[5] = 12.0 * first[5]
            for turn in range(8):
                for c in range(6):
                    turned = pltpu.roll(first[c], 8 - turn, 0) if turn else first[c]
                    first_kept[tile, rows_from(turn * 48 + c * 8), :] = turned
            image = jnp.broadcast_to(pair_ref[2:3, here], (8, LANES))
            step_y = jnp.where(image >= 6, 1.0, jnp.where(image >= 3, 0.0, -1.0))
            step_z = image.astype(jnp.float32) - 3.0 * step_y - 4.0
            first_kept[tile, rows_from(408), :] = step_y * box_y
            first_kept[tile, rows_from(416), :] = step_z * box_z
            words = [jnp.broadcast_to(word_ref[w : w + 1, here], (8, LANES)) for w in range(4)]
            low = jnp.where(sublane < 2, words[0], words[1])
            high = jnp.where(sublane < 6, words[2], words[3])
            bits = jnp.where(sublane < 4, low, high) >> (8 * (sublane & 1))
            bits = jnp.where(at + lane < total, bits, 0)
            for turn in range(8):
                turned = pltpu.roll(bits, 8 - turn, 0) if turn else bits
                wanted = (turned & (1 << sublane)) != 0
                far_kept[tile, rows_from(turn * 8), :] = jnp.where(wanted, 0.0, FAR_AWAY)
                term_kept[tile, rows_from(turn * 8), :] = jnp.where(wanted, reaction_term, 0.0)
        return carry

    lax.fori_loop(0, pairs // LANES // group_parts, prepare, 0)
    for copy in inward[7:]:
        copy.wait()
    energy = velocity_ref[...] * velocity_ref[...] / param_ref[3:4, :]
    energy = 0.5 * jnp.sum(energy, axis=1, keepdims=True)
    place_ref[...] = jnp.full_like(place_ref, -1)
    for start in range(0, far_count, LANES):
        width = min(LANES, far_count - start)
        chosen = halo_ref[0:1, start : start + width].astype(jnp.float32)
        for base in range(0, clusters, LANES):
            height = min(LANES, clusters - base)
            wanted = lax.broadcasted_iota(jnp.int32, (LANES, width), 0).astype(jnp.float32) + base
            hit = jnp.where(jnp.broadcast_to(chosen, (LANES, width)) == wanted, 1.0, 0.0)
            column = lax.broadcasted_iota(jnp.int32, (8, width), 1).astype(jnp.float32)
            found = lax.dot_general(
                jnp.concatenate([column + 1.0, jnp.zeros((8, width), jnp.float32)], axis=0).astype(jnp.bfloat16),
                hit.astype(jnp.bfloat16), (((1,), (1,)), ((), ())), preferred_element_type=jnp.float32,
            )[0:8].astype(jnp.int32)
            held = place_ref[:, base : base + LANES]
            place_ref[:, base : base + LANES] = jnp.where(found > 0, found - 1 + start, held)

    for copy in outward:
        copy.wait()
    near_lift = jnp.where(me >= count - 1, box_ref[0], 0.0)
    far_lift = jnp.where(me >= count - 2, box_ref[0], 0.0)
    upper = lax.broadcasted_iota(jnp.int32, (48, clusters), 0) < 8
    table_ref[:, clusters : 2 * clusters] = near_got[:, 0:clusters] + jnp.where(upper, near_lift, 0.0)
    upper = lax.broadcasted_iota(jnp.int32, (48, far_count), 0) < 8
    table_ref[:, 2 * clusters : slots] = far_got[:, 0:far_count] + jnp.where(upper, far_lift, 0.0)

    def fetch(number, part, slot):
        at = pl.multiple_of(number * block + part * LANES, LANES)
        here = pl.ds(at, LANES)
        tile = number * parts + part
        second = picked_rows(
            table_ref, jnp.broadcast_to(pair_ref[1:2, here], (8, LANES)), 0, second_tiles
        )
        for c in range(3):
            second[c] = second[c] - first_kept[tile, rows_from(384 + c * 8), :]
            if c:
                second[c] = second[c] + first_kept[tile, rows_from(400 + c * 8), :]
        for c in range(6):
            second_got[slot * 48 + c * 8 : slot * 48 + c * 8 + 8, :] = second[c]

    def interact(number, part):
        tile = number * parts + part
        low = (part % 2) * 48
        second = [second_got[low + c * 8 : low + c * 8 + 8, :] for c in range(6)]
        from_first = [None] * 3
        onto_second = [None] * 3
        for turn in range(7, -1, -1):
            first = [first_kept[tile, rows_from(turn * 48 + c * 8), :] for c in range(6)]
            delta = [second[c] - first[c] for c in range(3)]
            radius_sq = delta[0] * delta[0] + delta[1] * delta[1] + delta[2] * delta[2]
            inverse = lax.rsqrt(radius_sq + far_kept[tile, rows_from(turn * 8), :])
            inverse_sq = inverse * inverse
            cube = inverse * inverse_sq
            six = cube * cube
            scalar = first[3] * second[3] * (cube - term_kept[tile, rows_from(turn * 8), :]) + (
                first[5] * second[5] * six - first[4] * second[4]
            ) * (six * inverse_sq)
            for c in range(3):
                force = scalar * delta[c]
                if onto_second[c] is None:
                    from_first[c] = force
                    onto_second[c] = force
                else:
                    from_first[c] = pltpu.roll(from_first[c], 1, 0) + force
                    onto_second[c] = onto_second[c] + force
        for c in range(3):
            first_terms[part * 24 + c * 8 : part * 24 + c * 8 + 8, :] = from_first[c]
            second_terms[part * 24 + c * 8 : part * 24 + c * 8 + 8, :] = onto_second[c]
        return [onto_second[c] * second[c] - from_first[c] * first[c] for c in range(3)]

    def spread(number):
        for target, terms, row, hots, tiles in (
            (own_ref, first_terms, 0, first_hot, first_tiles),
            (other_ref, second_terms, 1, second_hot, second_tiles),
        ):
            rows = []
            columns = []
            for part in range(parts):
                at = pl.multiple_of(number * block + part * LANES, LANES)
                home = jnp.broadcast_to(pair_ref[row : row + 1, pl.ds(at, LANES)] >> LANE_BITS, (16, LANES))
                home = home.astype(jnp.float32).astype(jnp.bfloat16)
                home = jnp.concatenate([home] * 3, axis=0)
                pieces = split_two(terms[part * 24 : part * 24 + 24, :])
                rows.append(jnp.concatenate([
                    jnp.where(home == jnp.bfloat16(tile), pieces, jnp.bfloat16(0)) for tile in range(tiles)
                ], axis=0))
                columns.append(hots[number * parts + part, :, :])
            target[...] += lax.dot_general(
                jnp.concatenate(columns, axis=1), jnp.concatenate(rows, axis=1),
                (((1,), (1,)), ((), ())), preferred_element_type=jnp.float32,
            )

    fetch(0, 0, 0)

    def one_block(number, carry):
        spread(jnp.maximum(number - 1, 0))
        upcoming = jnp.minimum(number + 1, blocks - 1)
        virial = [virial_ref[c * 8 : c * 8 + 8, :] for c in range(3)]
        for part in range(parts):
            if part + 1 < parts:
                fetch(number, part + 1, (part + 1) % 2)
            else:
                fetch(upcoming, 0, 0)
            added = interact(number, part)
            virial = [virial[c] + added[c] for c in range(3)]
        for c in range(3):
            virial_ref[c * 8 : c * 8 + 8, :] = virial[c]
        return carry

    lax.fori_loop(0, blocks, one_block, 0)
    row = jnp.zeros((1, LANES), jnp.float32)
    for c in range(3):
        added = jnp.sum(virial_ref[c * 8 : c * 8 + 8, :], axis=0, keepdims=True)
        row = jnp.where(lane[0:1] == c, jnp.sum(added, axis=1, keepdims=True) * -0.5, row)
        row = jnp.where(lane[0:1] == c + 3, energy[c : c + 1], row)
    sum_ref[...] = row
    spread(blocks - 1)

    def sum_copy(step, source):
        return pltpu.make_async_remote_copy(
            src_ref=sum_ref, dst_ref=all_sums.at[source],
            send_sem=give_sems.at[step], recv_sem=take_sems.at[source],
            device_id={"gx": lax.rem(me + step, count)}, device_id_type=pl.DeviceIdType.MESH,
        )

    def give(step, carry):
        sum_copy(step, me).start()
        return carry

    def take(step, carry):
        sum_copy(step, lax.rem(me + count - step, count)).wait()
        return carry

    def joined(ref, tiles):
        value = ref[...]
        wide = round_up(value.shape[1], LANES)
        if wide > value.shape[1]:
            value = jnp.concatenate([value, jnp.zeros((LANES, wide - value.shape[1]), jnp.float32)], axis=1)
        value = value.T
        return jnp.concatenate([
            value[tile * 48 : tile * 48 + 24, :] + value[tile * 48 + 24 : tile * 48 + 48, :]
            for tile in range(tiles)
        ], axis=1)

    other = joined(other_ref, second_tiles)
    own = joined(own_ref, first_tiles)
    near_push[:, 0:clusters] = other[:, clusters : 2 * clusters]
    far_push[:, 0:far_count] = other[:, 2 * clusters : slots]
    homeward = [remote(far_push, far_back, 3, 2), remote(near_push, near_back, 2, 1)]
    for copy in homeward:
        copy.start()
    lax.fori_loop(1, count, give, 0)
    all_sums[me] = sum_ref[...]
    folded_ref[:, 0:clusters] = other[:, 0:clusters] - own[:, 0:clusters]
    for copy in homeward:
        copy.wait()
    place = place_ref[...]
    for base in range(0, clusters, LANES):
        lanes = slice(base, base + LANES)
        index = place[:, lanes]
        within = (jnp.maximum(index, 0) & (LANES - 1)).astype(jnp.uint32)
        for c in range(3):
            rows8 = slice(c * 8, c * 8 + 8)
            value = folded_ref[rows8, lanes] + near_back[rows8, lanes]
            for tile in range(-(-far_count // LANES)):
                source = far_back[rows8, tile * LANES : (tile + 1) * LANES]
                picked = jnp.take_along_axis(source, within, axis=1, mode="promise_in_bounds")
                mine = (index >= tile * LANES) & (index < (tile + 1) * LANES)
                value = value + jnp.where(mine, picked, 0.0)
            folded_out[rows8, lanes] = value
    lax.fori_loop(1, count, take, 0)
    totals = lax.fori_loop(
        0, count, lambda source, held: held + all_sums[source], jnp.zeros((1, LANES), jnp.float32)
    )
    virial = [jnp.broadcast_to(totals[:, c : c + 1], (1, LANES)) for c in range(3)]
    kinetic = [jnp.broadcast_to(totals[:, c : c + 1], (1, LANES)) for c in range(3, 6)]
    energy = kinetic[0] + kinetic[1] + kinetic[2]
    volume = box_ref[0] * box_ref[1] * box_ref[2]
    ratio = 2.0 * energy / (3.0 * count * clusters * 8 * thermal_scale_unit)
    rate_out[3:4] = extended_ref[0] + reservoir_inertia_mass * (ratio - 1.0)
    for c in range(3):
        change = barostat_gain * (kinetic[c] - virial[c] - pressure_target * volume / 2.0) / (energy / 3.0)
        rate_out[c : c + 1] = extended_ref[1 + c] + change


def final_kernel(
    folded_ref, rate_ref, position_ref, velocity_ref, param_ref,
    force_out, velocity_out, position_out, coupling_out, *, clusters
):
    sublane = lax.broadcasted_iota(jnp.int32, (8, LANES), 0)
    lane = lax.broadcasted_iota(jnp.int32, (8, LANES), 1)
    wanted = sublane == (lane & 7)
    for c in range(3):
        for tile in range(clusters * 8 // LANES):
            at = tile * 16
            source = folded_ref[c * 8 : c * 8 + 8, at // LANES * LANES : at // LANES * LANES + LANES]
            index = (at % LANES + lane // 8).astype(jnp.uint32)
            picked = jnp.take_along_axis(source, index, axis=1, mode="promise_in_bounds")
            force_out[c : c + 1, tile * LANES : (tile + 1) * LANES] = jnp.sum(
                jnp.where(wanted, picked, 0.0), axis=0, keepdims=True
            )
    row = rate_ref[3:4, :]
    for c in range(3):
        row = jnp.where(lane[0:1] == c + 1, rate_ref[c : c + 1, :], row)
    coupling_out[...] = row[:, 0:4]
    rates = rate_ref[0:3, 0:1]
    damping = rate_ref[3:4, 0:1]
    velocity = velocity_ref[...]
    moved = velocity + time_step * (
        force_out[...] * param_ref[3:4, :] - (damping + rates) * velocity
    )
    velocity_out[...] = moved
    position_out[...] = position_ref[...] * (1.0 + time_step * rates) + time_step * moved


def on_device(
    positions,
    velocities,
    atom_params,
    pair_list,
    pair_count,
    exclusion,
    halo_far,
    box_lengths,
    extended_variables,
):
    clusters = positions.shape[1] // 8
    far_clusters = halo_far.shape[0]
    slots = 2 * clusters + far_clusters
    pairs = pair_list.shape[1]
    count = lax.axis_size("gx")
    block = next(b for b in (768, 512, 256) if pairs % b == 0)
    wide = round_up(clusters, LANES)
    wide_far = round_up(far_clusters, LANES)
    wide_slots = round_up(slots, LANES)
    vmem = pl.BlockSpec(memory_space=pltpu.VMEM)
    shape = jax.ShapeDtypeStruct(positions.shape, jnp.float32)
    f32 = lambda *dims: pltpu.VMEM(dims, jnp.float32)
    halo = halo_far[None, :]
    pinned = lambda array: pltpu.with_memory_space_constraint(array, pltpu.HBM)
    folded, rates = pl.pallas_call(
        functools.partial(step_kernel, count=count, clusters=clusters, slots=slots, block=block),
        name="step_kernel",
        out_shape=(
            jax.ShapeDtypeStruct((24, wide), jnp.float32), jax.ShapeDtypeStruct((4, LANES), jnp.float32)
        ),
        in_specs=[pl.BlockSpec(memory_space=pltpu.HBM)] * 9,
        out_specs=(vmem,) * 2,
        scratch_shapes=[
            pltpu.SMEM(box_lengths.shape, jnp.float32), pltpu.SMEM(extended_variables.shape, jnp.float32),
            pltpu.SMEM(pair_count.shape, jnp.int32),
            f32(*positions.shape), f32(*velocities.shape), f32(*atom_params.shape),
            pltpu.VMEM(pair_list.shape, jnp.int32), pltpu.VMEM(exclusion.shape, jnp.int32),
            pltpu.VMEM(halo.shape, jnp.int32),
            f32(48, wide_slots), f32(48, wide), f32(48, wide), f32(48, wide_far), f32(48, wide_far),
            f32(24, wide), f32(24, wide_far), f32(24, wide), f32(24, wide_far),
            f32(1, LANES), f32(count, 1, LANES),
            pltpu.VMEM((8, wide), jnp.int32), f32(24, wide),
            f32(pairs // LANES, 424, LANES), f32(pairs // LANES, 64, LANES), f32(pairs // LANES, 64, LANES),
pltpu.VMEM((pairs // LANES, LANES, LANES), jnp.bfloat16),
            pltpu.VMEM((pairs // LANES, LANES, LANES), jnp.bfloat16),
            f32(96, LANES), f32(block // LANES * 24, LANES), f32(block // LANES * 24, LANES),
            f32(LANES, wide // LANES * 48), f32(LANES, wide_slots // LANES * 48), f32(24, LANES),
            pltpu.SemaphoreType.DMA((9,)), pltpu.SemaphoreType.DMA((4,)), pltpu.SemaphoreType.DMA((4,)),
            pltpu.SemaphoreType.DMA((count,)), pltpu.SemaphoreType.DMA((count,)),
        ],
        compiler_params=pltpu.CompilerParams(
            collective_id=0, has_side_effects=True, vmem_limit_bytes=48 * 1024 * 1024
        ),
    )(
        pinned(box_lengths), pinned(extended_variables), pair_count, pinned(positions), pinned(velocities),
        pinned(atom_params), pinned(pair_list), pinned(exclusion), pinned(halo),
    )
    forces, new_velocities, new_positions, new_coupling = pl.pallas_call(
        functools.partial(final_kernel, clusters=clusters),
        name="final_kernel",
        out_shape=(shape,) * 3 + (jax.ShapeDtypeStruct((1, 4), jnp.float32),),
        in_specs=[vmem] * 5,
        out_specs=(vmem,) * 4,
        compiler_params=pltpu.CompilerParams(vmem_limit_bytes=4 * 1024 * 1024),
    )(folded, rates, positions, velocities, atom_params)
    return (forces, new_velocities, new_positions, new_coupling.reshape(4))


def solution(mesh):
    spread = P(None, ("rep", "gx"))
    return jax.shard_map(
        on_device,
        mesh=mesh,
        in_specs=(spread,) * 4 + (P(("rep", "gx")), spread, P(("rep", "gx")), P("rep"), P("rep")),
        out_specs=(spread,) * 3 + (P("rep"),),
        check_vma=False,
    )
```
